256 devices in a mesh: gx: 8 (over x, core), gy: 32 (over z, y).
Axes of the slice: x: 4, y: 4, z: 8, core: 2. Of those that a mesh axis runs over, the one named last changes fastest.
Arguments:
- first_image: float32 [64, 256, 128], P('gx', 'gy'), may hold values from -6 to 6
- second_image: float32 [64, 256, 128], P('gx', 'gy'), may hold values from -6 to 6
- start_flow: float32 [3, 64, 256, 128], P(None, 'gx', 'gy'), may hold values from -3 to 3
Outputs:
- flow: float32 [3, 64, 256, 128], P(None, 'gx', 'gy')
The draws below stay inside these ranges and needn't reach their ends.
All inputs are finite; a program needn't handle non-finite values.
Results may differ from the reference program's by a relative error of at most 0.0001.
Values sent between devices are 32-bit elements; how exact they have to be, the bound alone decides.
No kernel may reach another device: no remote copies, remote signals or barrier semaphores. Data moves between devices by JAX's collectives and lax.ppermute only.
A program may use at most 128 MiB of HBM per device.

```python
import jax
import jax.numpy as jnp
from jax import lax

SWEEPS = 4
COARSE_SWEEPS = 12
CYCLES = 2
NX = 64
NY = 256
NZ = 128


def steps_of(rng, extent, split, smallest, high):
    level = 1.0
    for position, parts in split:
        draws = jax.random.uniform(jax.random.fold_in(jax.random.fold_in(rng, 6), position), (parts,), jnp.float32, smallest / len(split), high / len(split))
        level = level * jnp.repeat(jnp.exp(draws), extent[position] // parts).reshape((-1,) + (1,) * (len(extent) - 1 - position))
    return level


def bell_draw(stream_key, dims, scale, reach, cuts=(), kind=jnp.bfloat16):
    gain = steps_of(stream_key, dims, cuts, -0.22, 0.18) if cuts else 1.0
    drawn = jax.random.normal(stream_key, dims, jnp.float32) * scale * gain
    return jnp.minimum(jnp.maximum(drawn, -reach), reach).astype(kind)


def setup_inputs(seed: int = 0) -> dict:
    splits = jax.random.split(jax.random.key(seed), 4)
    return {
        "first_image": bell_draw(splits[0], (NX, NY, NZ), 1.0, 6.0, ((0, 8), (1, 32)), jnp.float32),
        "second_image": bell_draw(splits[1], (NX, NY, NZ), 1.0, 6.0, ((0, 8), (1, 32)), jnp.float32),
        "start_flow": bell_draw(splits[2], (3, NX, NY, NZ), 0.5, 3.0, ((1, 8), (2, 32)), jnp.float32),
    }


damping = 0.6
smooth_weight = 2.0
edge_scale = 0.25
floor_grad = 0.5

def pad_cells(field):
    widths = [(0, 0)] * (field.ndim - 3) + [(1, 1)] * 3
    return jnp.pad(field, widths)

def neighbours(padded):
    return [padded[..., 2:, 1:-1, 1:-1], padded[..., :-2, 1:-1, 1:-1], padded[..., 1:-1, 2:, 1:-1], padded[..., 1:-1, :-2, 1:-1], padded[..., 1:-1, 1:-1, 2:], padded[..., 1:-1, 1:-1, :-2]]

def centre(padded):
    return padded[..., 1:-1, 1:-1, 1:-1]

def diffusivity(padded_flow):
    beside_all = neighbours(padded_flow)
    total = jnp.zeros(centre(padded_flow).shape[1:], padded_flow.dtype)
    for upper, lower in ((0, 1), (2, 3), (4, 5)):
        slope = 0.5 * (beside_all[upper] - beside_all[lower])
        total = total + lax.optimization_barrier(jnp.sum(slope * slope, axis=0))
    return lax.rsqrt(1.0 + total / edge_scale)

def motion_tensor(padded_images):
    mean_image = 0.5 * (padded_images[0] + padded_images[1])
    beside_all = neighbours(mean_image)
    slopes = [0.5 * (beside_all[0] - beside_all[1]), 0.5 * (beside_all[2] - beside_all[3]), 0.5 * (beside_all[4] - beside_all[5])]
    change = centre(padded_images[1]) - centre(padded_images[0])
    scale = 1.0 / (slopes[0] * slopes[0] + slopes[1] * slopes[1] + slopes[2] * slopes[2] + floor_grad)
    tensor = jnp.stack([scale * slopes[0] * slopes[0], scale * slopes[0] * slopes[1], scale * slopes[0] * slopes[2], scale * slopes[1] * slopes[1], scale * slopes[1] * slopes[2], scale * slopes[2] * slopes[2]])
    source = jnp.stack([-scale * slopes[0] * change, -scale * slopes[1] * change, -scale * slopes[2] * change])
    return (tensor, source)

def apply_sym(matrix, vector):
    first = matrix[0] * vector[0] + matrix[1] * vector[1] + matrix[2] * vector[2]
    second = matrix[1] * vector[0] + matrix[3] * vector[1] + matrix[4] * vector[2]
    third = matrix[2] * vector[0] + matrix[4] * vector[1] + matrix[5] * vector[2]
    return jnp.stack([first, second, third])

def inverse_sym(tensor, total):
    aaa = tensor[0] + total
    bbb = tensor[1]
    ccc = tensor[2]
    ddd = tensor[3] + total
    eee = tensor[4]
    fff = tensor[5] + total
    cof_a = ddd * fff - eee * eee
    cof_b = ccc * eee - bbb * fff
    cof_c = bbb * eee - ccc * ddd
    cof_d = aaa * fff - ccc * ccc
    cof_e = bbb * ccc - aaa * eee
    cof_f = aaa * ddd - bbb * bbb
    determinant = aaa * cof_a + bbb * cof_b + ccc * cof_c
    return jnp.stack([cof_a, cof_b, cof_c, cof_d, cof_e, cof_f]) / determinant

def prepare(tensor, padded_weight, scale):
    middle = centre(padded_weight)
    faces = [scale * 2.0 * middle * other / (middle + other) for other in neighbours(padded_weight)]
    total = faces[0] + faces[1] + faces[2] + faces[3] + faces[4] + faces[5]
    return (tensor, jnp.stack(faces), total, inverse_sym(tensor, total))

def inflow(padded_field, level):
    faces = level[1]
    beside_all = neighbours(padded_field)
    result = faces[0] * beside_all[0]
    for index in range(1, 6):
        result = result + faces[index] * beside_all[index]
    return result

def relaxed(field, padded_field, source, level):
    return (1.0 - damping) * field + damping * apply_sym(level[3], source + inflow(padded_field, level))

def residual(field, padded_field, source, level):
    return source + inflow(padded_field, level) - apply_sym(level[0], field) - level[2] * field

def restrict(field, ratio):
    front = field.shape[:-3]
    across, along, depth = field.shape[-3:]
    blocks = field.reshape(front + (across // ratio, ratio, along // ratio, ratio, depth // ratio, ratio))
    return lax.optimization_barrier(jnp.mean(blocks, axis=(-5, -3, -1)))

def refine(padded, axis, ratio):
    count = padded.shape[axis] - 2
    middle = lax.slice_in_dim(padded, 1, count + 1, axis=axis)
    below = lax.slice_in_dim(padded, 0, count, axis=axis)
    above = lax.slice_in_dim(padded, 2, count + 2, axis=axis)
    pieces = []
    for offset in range(ratio):
        shift = (offset + 0.5) / ratio - 0.5
        other = below if shift < 0 else above
        pieces.append((1.0 - abs(shift)) * middle + abs(shift) * other)
    stacked = jnp.stack(pieces, axis=axis + 1)
    shape = list(middle.shape)
    shape[axis] = count * ratio
    return stacked.reshape(shape)

def refine_cells(padded, ratio):
    for axis in (1, 2, 3):
        padded = refine(padded, axis, ratio)
    return padded

def reference(first_image, second_image, start_flow):
    tensor, source = motion_tensor(pad_cells(jnp.stack([first_image, second_image])))
    mid_tensor = restrict(tensor, 2)
    coarse_tensor = restrict(mid_tensor, 4)
    flow = start_flow
    for cycle in range(CYCLES):
        weight = diffusivity(pad_cells(flow))
        fine = prepare(tensor, pad_cells(weight), smooth_weight)
        for sweep in range(SWEEPS):
            flow = relaxed(flow, pad_cells(flow), source, fine)
        fine_rest = residual(flow, pad_cells(flow), source, fine)
        mid_weight = restrict(weight, 2)
        mid = prepare(mid_tensor, pad_cells(mid_weight), smooth_weight / 4.0)
        mid_source = restrict(fine_rest, 2)
        error = damping * apply_sym(mid[3], mid_source)
        for sweep in range(SWEEPS - 1):
            error = relaxed(error, pad_cells(error), mid_source, mid)
        mid_rest = residual(error, pad_cells(error), mid_source, mid)
        unit_weight = jnp.ones(coarse_tensor.shape[1:], coarse_tensor.dtype)
        coarse = prepare(coarse_tensor, pad_cells(unit_weight), smooth_weight / 64.0)
        coarse_source = restrict(mid_rest, 4)
        correction = damping * apply_sym(coarse[3], coarse_source)

        def coarse_turn(index, current):
            return relaxed(current, pad_cells(current), coarse_source, coarse)
        correction = lax.fori_loop(0, COARSE_SWEEPS - 1, coarse_turn, correction)
        error = error + refine_cells(pad_cells(correction), 4)
        for sweep in range(SWEEPS):
            error = relaxed(error, pad_cells(error), mid_source, mid)
        flow = flow + refine_cells(pad_cells(error), 2)
        for sweep in range(SWEEPS):
            flow = relaxed(flow, pad_cells(flow), source, fine)
    return flow
```

```python
import functools

import jax
import jax.numpy as jnp
from jax import lax
from jax.experimental import pallas as pl
from jax.experimental.pallas import tpu as pltpu
from jax.sharding import Mesh
from jax.sharding import PartitionSpec as P

SWEEPS = 4
COARSE_SWEEPS = 12
CYCLES = 2
GX = ("gx_0", "gx_1")
GY = ("gy_0", "gy_1")

damping = 0.6
smooth_weight = 2.0
floor_grad = 0.5

NX, NY = 64, 256
ROWS = 24
WIDE = 20
MROWS = 16


def roll(v, shift, axis):
    return pltpu.roll(v, shift % v.shape[axis], axis)


def iota(shape, dim):
    return lax.broadcasted_iota(jnp.int32, shape, dim)


def face(a, b, scale):
    summed = a + b
    return (2.0 * scale) * a * b / jnp.where(summed > 0.0, summed, 1.0)


def inverse_sym(tensor, total):
    aaa = tensor[0] + total
    bbb = tensor[1]
    ccc = tensor[2]
    ddd = tensor[3] + total
    eee = tensor[4]
    fff = tensor[5] + total
    cof_a = ddd * fff - eee * eee
    cof_b = ccc * eee - bbb * fff
    cof_c = bbb * eee - ccc * ddd
    cof_d = aaa * fff - ccc * ccc
    cof_e = bbb * ccc - aaa * eee
    cof_f = aaa * ddd - bbb * bbb
    determinant = aaa * cof_a + bbb * cof_b + ccc * cof_c
    share = jnp.where(total > 0.0, damping / determinant, 0.0)
    return [cof * share for cof in (cof_a, cof_b, cof_c, cof_d, cof_e, cof_f)]


def apply_sym(m, v):
    return [
        m[0] * v[0] + m[1] * v[1] + m[2] * v[2],
        m[1] * v[0] + m[3] * v[1] + m[4] * v[2],
        m[2] * v[0] + m[4] * v[1] + m[5] * v[2],
    ]


def inflow(here, above, below, fx_up, fx_down, fy, fz):
    return (
        fx_up * above
        + fx_down * below
        + fy * roll(here, -1, 0)
        + roll(fy * here, 1, 0)
        + fz * roll(here, -1, 1)
        + roll(fz * here, 1, 1)
    )


def total_of(fx_up, fx_down, fy, fz):
    return fx_up + fx_down + fy + roll(fy, 1, 0) + fz + roll(fz, 1, 1)


def loop(low, high, turn, unroll=1):
    def step(index, carry):
        turn(index)
        return carry

    lax.fori_loop(low, high, step, 0, unroll=unroll)


def sides(par, which, even, odd, shape):
    is_odd = (jnp.zeros(shape, jnp.int32) + (par[which] & 1)) == 1
    return (lambda a, b: jnp.where(is_odd, a, b)), (lambda a, b: jnp.where(is_odd, b, a))


def hat(distance):
    return jnp.maximum(1.0 - jnp.abs(distance), 0.0)


def dot(a, b):
    return jnp.dot(a, b, precision=lax.Precision.HIGHEST, preferred_element_type=jnp.float32)


def fine_sweep(source, target, low, high, lev, tens):
    def turn(x):
        fx_up, fx_down = lev[0, x], lev[0, x - 1]
        fy, fz = lev[1, x], lev[2, x]
        here = [source[c, x] for c in range(3)]
        flux = [
            tens[6 + c, x]
            + inflow(here[c], source[c, x + 1], source[c, x - 1], fx_up, fx_down, fy, fz)
            for c in range(3)
        ]
        step = apply_sym([lev[3 + k, x] for k in range(6)], flux)
        for c in range(3):
            target[c, x] = (1.0 - damping) * here[c] + step[c]

    loop(low, high, turn)


def widen_kernel(layers, par, own, xa, xb, out):
    shape = (8, 128)
    low_of, high_of = sides(par, 0, None, None, shape)
    for f in range(own.shape[0]):
        for k in range(layers):
            out[f, k] = low_of(xa[f, 8 - layers + k], xb[f, 8 - layers + k])
            out[f, layers + 8 + k] = high_of(xa[f, k], xb[f, k])
        for k in range(8):
            out[f, layers + k] = own[f, k]


def stack_rows(par, own, ya, yb, out, fields, offset=0):
    low_of, high_of = sides(par, 1, None, None, (8, 128))

    def turn(x):
        for f in range(fields):
            a, b = ya[f, x], yb[f, x]
            out[f, x + offset, 0:8] = low_of(a, b)
            out[f, x + offset, 8:16] = own[f, x]
            out[f, x + offset, 16:24] = high_of(a, b)

    loop(0, own.shape[1], turn)


def pre_kernel(first, *refs):
    if first:
        par, own, ya, yb, flow_out, msg, lev, tens, u0, u1, w, even, odd, sums = refs
    else:
        par, own, ya, yb, tens, flow_out, msg, lev, u0, u1, w, even, odd, sums = refs
    shape = (ROWS, 128)
    lane = iota(shape, 1)
    last, start = lane == 127, lane == 0
    stack_rows(par, own, ya, yb, u0, own.shape[0])

    def z_slope(v):
        return jnp.where(last, 0.0, roll(v, -1, 1)) - jnp.where(start, 0.0, roll(v, 1, 1))

    def y_slope(v):
        return roll(v, -1, 0) - roll(v, 1, 0)

    if first:

        def tensor_turn(x):
            mean = 0.5 * (u0[3, x] + u0[4, x])
            sx = 0.25 * ((u0[3, x + 1] + u0[4, x + 1]) - (u0[3, x - 1] + u0[4, x - 1]))
            sy = 0.5 * y_slope(mean)
            sz = 0.5 * z_slope(mean)
            change = u0[4, x] - u0[3, x]
            scale = 1.0 / (sx * sx + sy * sy + sz * sz + floor_grad)
            gx, gy, gz = scale * sx, scale * sy, scale * sz
            for k, v in enumerate((gx * sx, gx * sy, gx * sz, gy * sy, gy * sz, gz * sz)):
                tens[k, x] = v
            for k, v in enumerate((gx, gy, gz)):
                tens[6 + k, x] = -v * change

        loop(2, 18, tensor_turn)

    row = iota(shape, 0) + (par[1] * 8 - 8)
    inside_y = (row >= 0) & (row < NY)

    def weight_turn(x):
        total = jnp.ones(shape, jnp.float32)
        for c in range(3):
            v = u0[c, x]
            for slope in (u0[c, x + 1] - u0[c, x - 1], y_slope(v), z_slope(v)):
                total = total + slope * slope
        place = x + (par[0] * 8 - 6)
        keep = jnp.where((place >= 0) & (place < NX), 1.0, 0.0)
        w[x] = jnp.where(inside_y, lax.rsqrt(total), 0.0) * keep

    loop(1, 19, weight_turn)

    def face_turn(x):
        v = w[x]
        lev[0, x] = face(v, w[x + 1], smooth_weight)
        lev[1, x] = face(v, roll(v, -1, 0), smooth_weight)
        lev[2, x] = jnp.where(last, 0.0, face(v, roll(v, -1, 1), smooth_weight))

    loop(1, 18, face_turn)

    def inverse_turn(x):
        total = total_of(lev[0, x], lev[0, x - 1], lev[1, x], lev[2, x])
        for k, v in enumerate(inverse_sym([tens[k, x] for k in range(6)], total)):
            lev[3 + k, x] = v

    loop(2, 18, inverse_turn)
    bufs = (u0, u1)
    for n in range(SWEEPS):
        fine_sweep(bufs[n % 2], bufs[(n + 1) % 2], 2 + n, 18 - n, lev, tens)

    def rest_at(x):
        fx_up, fx_down = lev[0, x], lev[0, x - 1]
        fy, fz = lev[1, x], lev[2, x]
        total = total_of(fx_up, fx_down, fy, fz)
        here = [u0[c, x] for c in range(3)]
        moved = apply_sym([tens[k, x] for k in range(6)], here)
        return [
            (
                tens[6 + c, x]
                + inflow(here[c], u0[c, x + 1], u0[c, x - 1], fx_up, fx_down, fy, fz)
                - moved[c]
                - total * here[c]
            )[8:16]
            for c in range(3)
        ]

    def rest_turn(m):
        x = 6 + 2 * m
        rest = [a + b for a, b in zip(rest_at(x), rest_at(x + 1))]
        pair = w[x] + w[x + 1]
        fields = rest + [pair[8:16], roll(pair, 2, 0)[8:16], pair[16:24]]
        if first:
            fields += [tens[k, x, 8:16] + tens[k, x + 1, 8:16] for k in range(6)]
        for k, v in enumerate(fields):
            stage = odd if k % 2 else even
            stage[pl.ds(pl.multiple_of((k // 2) * 32 + m * 8, 8), 8), :] = v

    loop(0, 4, rest_turn)
    for c in range(3):
        for k in range(8):
            flow_out[c, k] = u0[c, 6 + k, 8:16]
    square = (128, 128)
    into = iota(square, 0) // 2
    low = jnp.where(into == iota(square, 1), 0.125, 0.0)
    high = jnp.where(into + 64 == iota(square, 1), 0.125, 0.0)
    sums[...] = dot(even[...], low) + dot(odd[...], high)
    pairs = even.shape[0] // 32
    size = msg.shape[1]
    at = 0
    for p in range(pairs):
        if p == 2:
            v = sums[pl.ds(64, 4, stride=8), :] + sums[pl.ds(65, 4, stride=8), :]
            for s in range(8):
                msg[s, size - 8 : size - 4] = v
                msg[s, size - 4 : size] = v
            continue
        v = sums[pl.ds(p * 32, 16, stride=2), :] + sums[pl.ds(p * 32 + 1, 16, stride=2), :]
        for s in range(8):
            msg[s, at : at + 16] = v
        at += 16


def mid_sweep(source, target, mfx, mlev):
    def turn(x):
        fx_up, fx_down = mfx[x + 1], mfx[x]
        fy, fz = mlev[0, x], mlev[1, x]
        here = [source[c, x + 1] for c in range(3)]
        flux = [
            mlev[8 + c, x]
            + inflow(here[c], source[c, x + 2], source[c, x], fx_up, fx_down, fy, fz)
            for c in range(3)
        ]
        step = apply_sym([mlev[2 + k, x] for k in range(6)], flux)
        for c in range(3):
            target[c, x + 1] = (1.0 - damping) * here[c] + step[c]

    loop(0, 16, turn, unroll=2)
    seam(target)


def seam(field):
    for c in range(3):
        field[c, 0] = roll(field[c, 16], 64, 1)
        field[c, 17] = roll(field[c, 1], 64, 1)


def mid_kernel(first, *refs):
    if first:
        par, own, ya, yb, msg, edge, mfx, mlev, err, mtens, u1, w, stage = refs
    else:
        par, own, ya, yb, mtens, msg, edge, mfx, mlev, err, u1, w, stage = refs
    shape = (MROWS, 128)
    lane = iota(shape, 1)
    left = iota((8, 128), 1) < 64
    low_of, high_of = sides(par, 1, None, None, (8, 128))
    size = own.shape[1]
    zero4 = jnp.zeros((4, 128), jnp.float32)

    def split(a, b, which):
        if which:
            return jnp.where(left, roll(a, 64, 1), b)
        return jnp.where(left, a, roll(b, 64, 1))

    def fields_of(out, slot, pair, which):
        def turn(a):
            for kk in range(2):
                rows = slice(pair * 16 + kk * 8, pair * 16 + kk * 8 + 8)
                la, lb = low_of(ya[a, rows], yb[a, rows]), low_of(ya[a + 4, rows], yb[a + 4, rows])
                ha, hb = high_of(ya[a, rows], yb[a, rows]), high_of(ya[a + 4, rows], yb[a + 4, rows])
                for base, va, vb in ((1, la, lb), (5, own[a, rows], own[a + 4, rows]), (9, ha, hb)):
                    v = split(va, vb, which)
                    for k in range(2):
                        x = a * 4 + kk * 2 + k
                        if slot is None:
                            out[x, base : base + 4] = v[4 * k : 4 * k + 4]
                        else:
                            out[slot, x, base : base + 4] = v[4 * k : 4 * k + 4]

        loop(0, 4, turn)

    def clear_turn(x):
        for ref in (w,):
            ref[x, 0:1] = zero4[0:1]
            ref[x, 13:16] = zero4[0:3]
        for k in range(3):
            mlev[8 + k, x, 0:1] = zero4[0:1]
            mlev[8 + k, x, 13:16] = zero4[0:3]
        if first:
            for k in range(6):
                mtens[k, x, 0:1] = zero4[0:1]
                mtens[k, x, 13:16] = zero4[0:3]

    loop(0, 16, clear_turn)
    fields_of(mlev, 8, 0, 0)
    fields_of(mlev, 9, 0, 1)
    fields_of(mlev, 10, 1, 0)
    fields_of(w, None, 1, 1)
    if first:
        for k in range(6):
            fields_of(mtens, k, 2 + k // 2, k % 2)
    outer = slice(size - 8, size)
    for a in range(4):
        la, lb = low_of(ya[a, outer], yb[a, outer]), low_of(ya[a + 4, outer], yb[a + 4, outer])
        ha, hb = high_of(ya[a, outer], yb[a, outer]), high_of(ya[a + 4, outer], yb[a + 4, outer])
        lo, hi = split(la, lb, 0), split(ha, hb, 1)
        for k in range(4):
            w[a * 4 + k, 0:1] = lo[k : k + 1]
            w[a * 4 + k, 13:14] = hi[k : k + 1]

    scale = smooth_weight / 4.0
    stop = (lane == 63) | (lane == 127)

    def face_turn(x):
        v = w[x]
        mlev[0, x] = face(v, roll(v, -1, 0), scale)
        mlev[1, x] = jnp.where(stop, 0.0, face(v, roll(v, -1, 1), scale))

    loop(0, 16, face_turn)

    def across_turn(x):
        mfx[x + 1] = face(w[x], w[x + 1], scale)

    loop(0, 15, across_turn)
    seam_face = jnp.where(lane < 64, face(w[15], roll(w[0], 64, 1), scale), 0.0)
    mfx[16] = seam_face
    mfx[0] = roll(seam_face, 64, 1)

    def inverse_turn(x):
        total = total_of(mfx[x + 1], mfx[x], mlev[0, x], mlev[1, x])
        inv = inverse_sym([mtens[k, x] for k in range(6)], total)
        for k in range(6):
            mlev[2 + k, x] = inv[k]
        begin = apply_sym(inv, [mlev[8 + c, x] for c in range(3)])
        for c in range(3):
            u1[c, x + 1] = begin[c]

    loop(0, 16, inverse_turn)
    seam(u1)
    bufs = (u1, err)
    for n in range(SWEEPS - 1):
        mid_sweep(bufs[n % 2], bufs[(n + 1) % 2], mfx, mlev)
    count = stage.shape[0] // 4
    stage[...] = jnp.zeros(stage.shape, jnp.float32)

    def rest_turn(a):
        sums = [jnp.zeros(shape, jnp.float32) for _ in range(9 if first else 3)]
        for k in range(4):
            x = a * 4 + k
            fx_up, fx_down = mfx[x + 1], mfx[x]
            fy, fz = mlev[0, x], mlev[1, x]
            total = total_of(fx_up, fx_down, fy, fz)
            here = [err[c, x + 1] for c in range(3)]
            moved = apply_sym([mtens[k, x] for k in range(6)], here)
            for c in range(3):
                sums[c] = sums[c] + (
                    mlev[8 + c, x]
                    + inflow(here[c], err[c, x + 2], err[c, x], fx_up, fx_down, fy, fz)
                    - moved[c]
                    - total * here[c]
                )
            if first:
                for q in range(6):
                    sums[3 + q] = sums[3 + q] + mtens[q, x]
        for q, v in enumerate(sums):
            stage[pl.ds(a * count + q, 1), :] = jnp.sum(v[5:9], axis=0, keepdims=True)

    loop(0, 4, rest_turn)
    for c in range(3):
        for x in range(16):
            edge[c, x] = err[c, x + 1, 5:9]
    square = (128, 128)
    z, to = iota(square, 0), iota(square, 1)
    gather = jnp.where((z // 64 == to // 64) & ((z % 64) // 4 == to % 64), 1.0 / 64.0, 0.0)
    mixed = dot(stage[...], gather)
    value = mixed[0:count]
    for a in range(1, 4):
        value = value + roll(mixed[a * count : (a + 1) * count], 16 * a, 1)
    for s in range(32):
        msg[s] = value


def coarse_kernel(first, *refs):
    if first:
        par, whole, mfx, mlev, err, ea, eb, out, cinv, u0, u1, lifted = refs
    else:
        par, whole, mfx, mlev, err, ea, eb, cinv, out, u0, u1, lifted = refs
    count = whole.shape[0] // 32
    grid = (32, 128)
    row, lane = iota(grid, 0), iota(grid, 1)
    cx, cz = lane // 16, lane % 16
    scale = smooth_weight / 64.0
    one = lambda cond: jnp.where(cond, scale, 0.0)
    ups = (one(cx < 7), one(cx > 0), one(row < 31), one(row > 0), one(cz < 15), one(cz > 0))
    total = ups[0] + ups[1] + ups[2] + ups[3] + ups[4] + ups[5]
    if first:
        inv = inverse_sym([whole[pl.ds(3 + k, 32, stride=count), :] for k in range(6)], total)
        for k in range(6):
            cinv[k] = inv[k]
    inv = [cinv[k] for k in range(6)]
    source = [whole[pl.ds(c, 32, stride=count), :] for c in range(3)]

    def turn(index, now):
        flux = []
        for c in range(3):
            v = now[c]
            flux.append(
                source[c]
                + ups[0] * roll(v, -16, 1)
                + ups[1] * roll(v, 16, 1)
                + ups[2] * roll(v, -1, 0)
                + ups[3] * roll(v, 1, 0)
                + ups[4] * roll(v, -1, 1)
                + ups[5] * roll(v, 1, 1)
            )
        step = apply_sym(inv, flux)
        return tuple((1.0 - damping) * now[c] + step[c] for c in range(3))

    correction = lax.fori_loop(0, COARSE_SWEEPS - 1, turn, tuple(apply_sym(inv, source)))

    shape = (MROWS, 32)
    place = (iota(shape, 0) + (par[1] * 4 - 5)).astype(jnp.float32) * 0.25 - 0.375
    along = hat(place - iota(shape, 1).astype(jnp.float32))
    rows = jnp.concatenate([dot(along, correction[c]) for c in range(3)], axis=0)
    square = (128, 128)
    src, to = iota(square, 0), iota(square, 1)
    depth = hat((to % 64).astype(jnp.float32) * 0.25 - 0.375 - (src % 16).astype(jnp.float32))
    for a in range(4):
        spread = jnp.where(src // 16 == a + 4 * (to // 64), depth, 0.0)
        lifted[a + 1] = dot(rows, spread)
    halves = iota((3 * MROWS, 128), 1) < 64
    lifted[0] = jnp.where(halves, 0.0, roll(lifted[4], 64, 1))
    lifted[5] = jnp.where(halves, roll(lifted[1], 64, 1), 0.0)

    low_of, high_of = sides(par, 1, None, None, (4, 128))
    zero = jnp.zeros((MROWS, 128), jnp.float32)
    for x in range(16):
        a, d = x // 4, x % 4
        t = (d + 0.5) / 4 - 0.5
        other = a if t < 0 else a + 2
        added = (1.0 - abs(t)) * lifted[a + 1] + abs(t) * lifted[other]
        for c in range(3):
            u0[c, x + 1] = zero
            u0[c, x + 1, 1:5] = low_of(ea[c, x], eb[c, x])
            u0[c, x + 1, 5:9] = err[c, x + 1, 5:9]
            u0[c, x + 1, 9:13] = high_of(ea[c, x], eb[c, x])
            u0[c, x + 1] = u0[c, x + 1] + added[c * MROWS : (c + 1) * MROWS]
    seam(u0)
    bufs = (u0, u1)
    for n in range(SWEEPS):
        mid_sweep(bufs[n % 2], bufs[(n + 1) % 2], mfx, mlev)

    left = iota((4, 128), 1) < 64
    for b in range(3):
        block = par[0] + (b - 1)
        there = jnp.where((block >= 0) & (block < 8), 1.0, 0.0)
        block = jnp.clip(block, 0, 7)
        upper = (jnp.zeros((4, 128), jnp.int32) + block // 4) == 1
        for k in range(4):
            x = (block % 4) * 4 + k + 1
            v = [u0[c, x, 5:9] for c in range(3)]
            v = [(a, roll(a, 64, 1)) for a in v]
            to_left = [jnp.where(upper, turned, a) for a, turned in v]
            to_right = [jnp.where(upper, a, turned) for a, turned in v]
            out[0, b * 4 + k] = jnp.where(left, to_left[0], to_right[1]) * there
            out[1, b * 4 + k] = jnp.where(left, to_left[2], 0.0) * there


def post_kernel(par, own, ya, yb, mine, ea, eb, lev, tens, out, u0, u1, mixed, lifted, tall):
    stack_rows(par, own, ya, yb, u0, 3, 2)
    low_of, high_of = sides(par, 1, None, None, (4, 128))
    zero = jnp.zeros((4, 128), jnp.float32)
    for x in range(12):
        for p in range(2):
            v = [low_of(ea[p, x], eb[p, x]), mine[p, x], high_of(ea[p, x], eb[p, x])]
            for q in range(3):
                mixed[2 * p, x, 4 * q : 4 * q + 4] = v[q]
            mixed[2 * p, x, 12:16] = zero
    square = (128, 128)
    src, to = iota(square, 0), iota(square, 1)
    place = to.astype(jnp.float32) * 0.5 - 0.25
    depth = hat(place - (src % 64).astype(jnp.float32))
    low = jnp.where(src < 64, depth, 0.0)
    high = jnp.where(src < 64, 0.0, depth)
    for c in range(3):
        v = mixed[2 * (c // 2)].reshape(12 * 16, 128)
        lifted[c] = dot(v, high if c == 1 else low).reshape(12, 16, 128)

    def tall_turn(x):
        for c in range(3):
            v = lifted[c, x]
            tall[c, x, pl.ds(0, 12, stride=2), :] = (0.75 * v + 0.25 * roll(v, 1, 0))[0:12]
            tall[c, x, pl.ds(1, 12, stride=2), :] = (0.75 * v + 0.25 * roll(v, -1, 0))[0:12]

    loop(0, 12, tall_turn)

    def add_turn(m):
        for c in range(3):
            a, b, d = tall[c, m - 1], tall[c, m], tall[c, m + 1]
            x = 2 * m - 2
            u0[c, x] = u0[c, x] + (0.75 * b + 0.25 * a)
            u0[c, x + 1] = u0[c, x + 1] + (0.75 * b + 0.25 * d)

    loop(2, 10, add_turn)
    bufs = (u0, u1)
    for n in range(SWEEPS):
        fine_sweep(bufs[n % 2], bufs[(n + 1) % 2], 3 + n, 17 - n, lev, tens)
    for c in range(3):
        for k in range(8):
            out[c, k] = u0[c, 6 + k, 8:16]


def f32(*shape):
    return jax.ShapeDtypeStruct(shape, jnp.float32)


def call(kernel, name, outs, scratch, args):
    specs = [pl.BlockSpec(memory_space=pltpu.SMEM)]
    specs += [pl.BlockSpec(memory_space=pltpu.VMEM)] * (len(args) - 1)
    return pl.pallas_call(
        kernel,
        name=name,
        in_specs=specs,
        out_specs=[pl.BlockSpec(memory_space=pltpu.VMEM)] * len(outs),
        out_shape=[f32(*shape) for shape in outs],
        scratch_shapes=[pltpu.VMEM(shape, jnp.float32) for shape in scratch],
        cost_estimate=pl.CostEstimate(flops=20_000_000, bytes_accessed=1_000_000, transcendentals=0),
    )(*args)


def pairs_of(size, start):
    pairs = []
    for k in range(start, size - 1, 2):
        pairs += [(k, k + 1), (k + 1, k)]
    return pairs


def beside(field, axes):
    size = lax.axis_size(axes)
    return [lax.ppermute(field, axes, pairs_of(size, start)) for start in (0, 1)]


def shared(message, axes):
    return lax.all_to_all(message, axes, 0, 0, tiled=True)


def body(first_image, second_image, start_flow):
    par = jnp.stack([lax.axis_index(GX), lax.axis_index(GY)]).astype(jnp.int32)
    block = jnp.concatenate([start_flow, first_image[None], second_image[None]])
    flow = start_flow
    tens = mtens = cinv = None
    fine_shape, mid_shape = (WIDE, ROWS, 128), (16, MROWS, 128)
    for cycle in range(CYCLES):
        first = cycle == 0
        sent = block if first else flow
        fields = sent.shape[0]
        (wide,) = call(
            functools.partial(widen_kernel, 6), f"widen{cycle}", [(fields, WIDE, 8, 128)], [], [par, sent, *beside(sent, GX)]
        )
        size = 88 if first else 40
        stage = (6 if first else 3) * 32
        outs = [(3, 8, 8, 128), (8, size, 128), (9, *fine_shape)]
        scratch = [(fields, *fine_shape), (3, *fine_shape), fine_shape, (stage, 128), (stage, 128), (stage, 128)]
        args = [par, wide, *beside(wide, GY)]
        pre = functools.partial(pre_kernel, first)
        if first:
            flow, message, lev, tens = call(pre, "pre0", [*outs, (9, *fine_shape)], scratch, args)
        else:
            flow, message, lev = call(pre, "pre1", outs, scratch, [*args, tens])
        mids = shared(message, GX)
        args = [par, mids, *beside(mids, GY)]
        count = 16 if first else 8
        outs = [(32, count, 128), (3, 16, 4, 128), (17, MROWS, 128), (11, *mid_shape), (3, 18, MROWS, 128)]
        scratch = [(3, 18, MROWS, 128), mid_shape, (4 * count, 128)]
        mid = functools.partial(mid_kernel, first)
        if first:
            coarse, edge, mfx, mlev, err, mtens = call(mid, "mid0", [*outs, (6, *mid_shape)], scratch, args)
        else:
            coarse, edge, mfx, mlev, err = call(mid, "mid1", outs, scratch, [*args, mtens])
        (wide,) = call(functools.partial(widen_kernel, 4), f"widen{cycle}b", [(3, 16, 8, 128)], [], [par, flow, *beside(flow, GX)])
        flows = [wide, *beside(wide, GY)]
        whole = shared(coarse, GY).reshape(32 * count, 128)
        args = [par, whole, mfx, mlev, err, *beside(edge, GY)]
        outs = [(2, 12, 4, 128)]
        scratch = [(3, 18, MROWS, 128), (3, 18, MROWS, 128), (6, 3 * MROWS, 128)]
        low = functools.partial(coarse_kernel, first)
        if first:
            error, cinv = call(low, "coarse0", [*outs, (6, 32, 128)], scratch, args)
        else:
            (error,) = call(low, "coarse1", outs, scratch, [*args, cinv])
        args = [par, *flows, error, *beside(error, GY), lev, tens]
        scratch = [(3, *fine_shape), (3, *fine_shape), (3, 12, 16, 128), (3, 12, 16, 128), (3, 12, 24, 128)]
        (flow,) = call(post_kernel, f"post{cycle}", [(3, 8, 8, 128)], scratch, args)
    return flow


def solution(mesh):
    finer = Mesh(mesh.devices.reshape(4, 2, 8, 4), ("gx_0", "gx_1", "gy_0", "gy_1"))
    return jax.shard_map(
        body,
        mesh=finer,
        in_specs=(P(GX, GY, None), P(GX, GY, None), P(None, GX, GY, None)),
        out_specs=P(None, GX, GY, None),
        check_vma=False,
    )
```

```python
import functools

import jax
import jax.numpy as jnp
from jax import lax
from jax.experimental import pallas as pl
from jax.experimental.pallas import tpu as pltpu
from jax.sharding import Mesh
from jax.sharding import PartitionSpec as P


SWEEPS = 4
COARSE_SWEEPS = 12
CYCLES = 2
GX = ("gx_0", "gx_1")
GY = ("gy_0", "gy_1")

damping = 0.6
smooth_weight = 2.0
floor_grad = 0.5

NX, NY = 64, 256
ROWS = 24
WIDE = 20
MROWS = 16


def roll(v, shift, axis):
    return pltpu.roll(v, shift % v.shape[axis], axis)


def iota(shape, dim):
    return lax.broadcasted_iota(jnp.int32, shape, dim)


def face(a, b, scale):
    summed = a + b
    return (2.0 * scale) * a * b / jnp.where(summed > 0.0, summed, 1.0)


def inverse_sym(tensor, total):
    aaa = tensor[0] + total
    bbb = tensor[1]
    ccc = tensor[2]
    ddd = tensor[3] + total
    eee = tensor[4]
    fff = tensor[5] + total
    cof_a = ddd * fff - eee * eee
    cof_b = ccc * eee - bbb * fff
    cof_c = bbb * eee - ccc * ddd
    cof_d = aaa * fff - ccc * ccc
    cof_e = bbb * ccc - aaa * eee
    cof_f = aaa * ddd - bbb * bbb
    determinant = aaa * cof_a + bbb * cof_b + ccc * cof_c
    share = jnp.where(total > 0.0, damping / determinant, 0.0)
    return [cof * share for cof in (cof_a, cof_b, cof_c, cof_d, cof_e, cof_f)]


def apply_sym(m, v):
    return [
        m[0] * v[0] + m[1] * v[1] + m[2] * v[2],
        m[1] * v[0] + m[3] * v[1] + m[4] * v[2],
        m[2] * v[0] + m[4] * v[1] + m[5] * v[2],
    ]


def inflow(here, above, below, fx_up, fx_down, fy, fz):
    return (
        fx_up * above
        + fx_down * below
        + fy * roll(here, -1, 0)
        + roll(fy * here, 1, 0)
        + fz * roll(here, -1, 1)
        + roll(fz * here, 1, 1)
    )


def total_of(fx_up, fx_down, fy, fz):
    return fx_up + fx_down + fy + roll(fy, 1, 0) + fz + roll(fz, 1, 1)


def loop(low, high, turn, unroll=1):
    def step(index, carry):
        turn(index)
        return carry

    lax.fori_loop(low, high, step, 0, unroll=unroll)


def sides(par, which, shape):
    is_odd = (jnp.zeros(shape, jnp.int32) + (par[which] & 1)) == 1
    return (lambda a, b: jnp.where(is_odd, a, b)), (lambda a, b: jnp.where(is_odd, b, a))


def hat(distance):
    return jnp.maximum(1.0 - jnp.abs(distance), 0.0)


def dot(a, b):
    return jnp.dot(a, b, precision=lax.Precision.HIGHEST, preferred_element_type=jnp.float32)


def fine_sweep(source, target, low, high, lev, tens):
    def turn(x):
        fx_up, fx_down = lev[0, x], lev[0, x - 1]
        fy, fz = lev[1, x], lev[2, x]
        here = [source[c, x] for c in range(3)]
        flux = [
            tens[6 + c, x]
            + inflow(here[c], source[c, x + 1], source[c, x - 1], fx_up, fx_down, fy, fz)
            for c in range(3)
        ]
        step = apply_sym([lev[3 + k, x] for k in range(6)], flux)
        for c in range(3):
            target[c, x] = (1.0 - damping) * here[c] + step[c]

    loop(low, high, turn)


def widen_kernel(layers, par, own, xa, xb, out):
    shape = (8, 128)
    low_of, high_of = sides(par, 0, shape)
    for f in range(own.shape[0]):
        for k in range(layers):
            out[f, k] = low_of(xa[f, 8 - layers + k], xb[f, 8 - layers + k])
            out[f, layers + 8 + k] = high_of(xa[f, k], xb[f, k])
        for k in range(8):
            out[f, layers + k] = own[f, k]


def stack_rows(par, own, ya, yb, out, fields):
    low_of, high_of = sides(par, 1, (8, 128))

    def turn(x):
        for f in range(fields):
            a, b = ya[f, x], yb[f, x]
            out[f, x, 0:8] = low_of(a, b)
            out[f, x, 8:16] = own[f, x]
            out[f, x, 16:24] = high_of(a, b)

    loop(0, own.shape[1], turn)


def pre_kernel(first, *refs):
    if first:
        par, own, ya, yb, flow_out, msg, lev, tens, u0, u1, w, even, odd, sums = refs
    else:
        par, own, ya, yb, tens, flow_out, msg, lev, u0, u1, w, even, odd, sums = refs
    shape = (ROWS, 128)
    lane = iota(shape, 1)
    last, start = lane == 127, lane == 0
    stack_rows(par, own, ya, yb, u0, own.shape[0])

    def z_slope(v):
        return jnp.where(last, 0.0, roll(v, -1, 1)) - jnp.where(start, 0.0, roll(v, 1, 1))

    def y_slope(v):
        return roll(v, -1, 0) - roll(v, 1, 0)

    if first:

        def tensor_turn(x):
            mean = 0.5 * (u0[3, x] + u0[4, x])
            sx = 0.25 * ((u0[3, x + 1] + u0[4, x + 1]) - (u0[3, x - 1] + u0[4, x - 1]))
            sy = 0.5 * y_slope(mean)
            sz = 0.5 * z_slope(mean)
            change = u0[4, x] - u0[3, x]
            scale = 1.0 / (sx * sx + sy * sy + sz * sz + floor_grad)
            gx, gy, gz = scale * sx, scale * sy, scale * sz
            for k, v in enumerate((gx * sx, gx * sy, gx * sz, gy * sy, gy * sz, gz * sz)):
                tens[k, x] = v
            for k, v in enumerate((gx, gy, gz)):
                tens[6 + k, x] = -v * change

        loop(2, 18, tensor_turn)

    row = iota(shape, 0) + (par[1] * 8 - 8)
    inside_y = (row >= 0) & (row < NY)

    def weight_turn(x):
        total = jnp.ones(shape, jnp.float32)
        for c in range(3):
            v = u0[c, x]
            for slope in (u0[c, x + 1] - u0[c, x - 1], y_slope(v), z_slope(v)):
                total = total + slope * slope
        place = x + (par[0] * 8 - 6)
        keep = jnp.where((place >= 0) & (place < NX), 1.0, 0.0)
        w[x] = jnp.where(inside_y, lax.rsqrt(total), 0.0) * keep

    loop(1, 19, weight_turn)

    def face_turn(x):
        v = w[x]
        lev[0, x] = face(v, w[x + 1], smooth_weight)
        lev[1, x] = face(v, roll(v, -1, 0), smooth_weight)
        lev[2, x] = jnp.where(last, 0.0, face(v, roll(v, -1, 1), smooth_weight))

    loop(1, 18, face_turn)

    def inverse_turn(x):
        total = total_of(lev[0, x], lev[0, x - 1], lev[1, x], lev[2, x])
        for k, v in enumerate(inverse_sym([tens[k, x] for k in range(6)], total)):
            lev[3 + k, x] = v

    loop(2, 18, inverse_turn)
    bufs = (u0, u1)
    for n in range(SWEEPS):
        fine_sweep(bufs[n % 2], bufs[(n + 1) % 2], 2 + n, 18 - n, lev, tens)

    def rest_at(x):
        fx_up, fx_down = lev[0, x], lev[0, x - 1]
        fy, fz = lev[1, x], lev[2, x]
        total = total_of(fx_up, fx_down, fy, fz)
        here = [u0[c, x] for c in range(3)]
        moved = apply_sym([tens[k, x] for k in range(6)], here)
        return [
            (
                tens[6 + c, x]
                + inflow(here[c], u0[c, x + 1], u0[c, x - 1], fx_up, fx_down, fy, fz)
                - moved[c]
                - total * here[c]
            )[8:16]
            for c in range(3)
        ]

    def rest_turn(m):
        x = 6 + 2 * m
        rest = [a + b for a, b in zip(rest_at(x), rest_at(x + 1))]
        pair = w[x] + w[x + 1]
        fields = rest + [pair[8:16], roll(pair, 2, 0)[8:16], pair[16:24]]
        if first:
            fields += [tens[k, x, 8:16] + tens[k, x + 1, 8:16] for k in range(6)]
        for k, v in enumerate(fields):
            stage = odd if k % 2 else even
            stage[pl.ds(pl.multiple_of((k // 2) * 32 + m * 8, 8), 8), :] = v

    loop(0, 4, rest_turn)
    for c in range(3):
        for k in range(8):
            flow_out[c, k] = u0[c, 6 + k, 8:16]
    square = (128, 128)
    into = iota(square, 0) // 2
    low = jnp.where(into == iota(square, 1), 0.125, 0.0)
    high = jnp.where(into + 64 == iota(square, 1), 0.125, 0.0)
    sums[...] = dot(even[...], low) + dot(odd[...], high)
    pairs = even.shape[0] // 32
    size = msg.shape[1]
    at = 0
    for p in range(pairs):
        if p == 2:
            v = sums[pl.ds(64, 4, stride=8), :] + sums[pl.ds(65, 4, stride=8), :]
            for s in range(8):
                msg[s, size - 8 : size - 4] = v
                msg[s, size - 4 : size] = v
            continue
        v = sums[pl.ds(p * 32, 16, stride=2), :] + sums[pl.ds(p * 32 + 1, 16, stride=2), :]
        for s in range(8):
            msg[s, at : at + 16] = v
        at += 16


def wide_layers(par, own, xa, xb, place):
    low_of, high_of = sides(par, 0, (8, 128))
    for c in range(3):
        for k in range(4):
            place(c, k, low_of(xa[c, 4 + k], xb[c, 4 + k]))
            place(c, 12 + k, high_of(xa[c, k], xb[c, k]))
        for k in range(8):
            place(c, 4 + k, own[c, k])


def send_flow(par, flow, fa, fb, to_a, to_b):
    first_of, second_of = sides(par, 1, (4, 128))

    def place(c, k, v):
        to_a[c, k] = first_of(v[0:4], v[4:8])
        to_b[c, k] = second_of(v[0:4], v[4:8])

    wide_layers(par, flow, fa, fb, place)


def mid_sweep(source, target, mfx, mlev):
    def turn(x):
        fx_up, fx_down = mfx[x + 1], mfx[x]
        fy, fz = mlev[0, x], mlev[1, x]
        here = [source[c, x + 1] for c in range(3)]
        flux = [
            mlev[8 + c, x]
            + inflow(here[c], source[c, x + 2], source[c, x], fx_up, fx_down, fy, fz)
            for c in range(3)
        ]
        step = apply_sym([mlev[2 + k, x] for k in range(6)], flux)
        for c in range(3):
            target[c, x + 1] = (1.0 - damping) * here[c] + step[c]

    loop(0, 16, turn, unroll=2)
    seam(target)


def seam(field):
    for c in range(3):
        field[c, 0] = roll(field[c, 16], 64, 1)
        field[c, 17] = roll(field[c, 1], 64, 1)


def mid_kernel(first, *refs):
    if first:
        par, own, ya, yb, flow, fa, fb, msg, to_a, to_b, mfx, mlev, err, mtens, u1, w, stage = refs
    else:
        par, own, ya, yb, flow, fa, fb, mtens, msg, to_a, to_b, mfx, mlev, err, u1, w, stage = refs
    send_flow(par, flow, fa, fb, to_a, to_b)
    shape = (MROWS, 128)
    lane = iota(shape, 1)
    left = iota((8, 128), 1) < 64
    low_of, high_of = sides(par, 1, (8, 128))
    size = own.shape[1]
    zero4 = jnp.zeros((4, 128), jnp.float32)

    def split(a, b, which):
        if which:
            return jnp.where(left, roll(a, 64, 1), b)
        return jnp.where(left, a, roll(b, 64, 1))

    def fields_of(out, slot, pair, which):
        def turn(a):
            for kk in range(2):
                rows = slice(pair * 16 + kk * 8, pair * 16 + kk * 8 + 8)
                la, lb = low_of(ya[a, rows], yb[a, rows]), low_of(ya[a + 4, rows], yb[a + 4, rows])
                ha, hb = high_of(ya[a, rows], yb[a, rows]), high_of(ya[a + 4, rows], yb[a + 4, rows])
                for base, va, vb in ((1, la, lb), (5, own[a, rows], own[a + 4, rows]), (9, ha, hb)):
                    v = split(va, vb, which)
                    for k in range(2):
                        x = a * 4 + kk * 2 + k
                        if slot is None:
                            out[x, base : base + 4] = v[4 * k : 4 * k + 4]
                        else:
                            out[slot, x, base : base + 4] = v[4 * k : 4 * k + 4]

        loop(0, 4, turn)

    def clear_turn(x):
        for ref in (w,):
            ref[x, 0:1] = zero4[0:1]
            ref[x, 13:16] = zero4[0:3]
        for k in range(3):
            mlev[8 + k, x, 0:1] = zero4[0:1]
            mlev[8 + k, x, 13:16] = zero4[0:3]
        if first:
            for k in range(6):
                mtens[k, x, 0:1] = zero4[0:1]
                mtens[k, x, 13:16] = zero4[0:3]

    loop(0, 16, clear_turn)
    fields_of(mlev, 8, 0, 0)
    fields_of(mlev, 9, 0, 1)
    fields_of(mlev, 10, 1, 0)
    fields_of(w, None, 1, 1)
    if first:
        for k in range(6):
            fields_of(mtens, k, 2 + k // 2, k % 2)
    outer = slice(size - 8, size)
    for a in range(4):
        la, lb = low_of(ya[a, outer], yb[a, outer]), low_of(ya[a + 4, outer], yb[a + 4, outer])
        ha, hb = high_of(ya[a, outer], yb[a, outer]), high_of(ya[a + 4, outer], yb[a + 4, outer])
        lo, hi = split(la, lb, 0), split(ha, hb, 1)
        for k in range(4):
            w[a * 4 + k, 0:1] = lo[k : k + 1]
            w[a * 4 + k, 13:14] = hi[k : k + 1]

    scale = smooth_weight / 4.0
    stop = (lane == 63) | (lane == 127)

    def face_turn(x):
        v = w[x]
        mlev[0, x] = face(v, roll(v, -1, 0), scale)
        mlev[1, x] = jnp.where(stop, 0.0, face(v, roll(v, -1, 1), scale))

    loop(0, 16, face_turn)

    def across_turn(x):
        mfx[x + 1] = face(w[x], w[x + 1], scale)

    loop(0, 15, across_turn)
    seam_face = jnp.where(lane < 64, face(w[15], roll(w[0], 64, 1), scale), 0.0)
    mfx[16] = seam_face
    mfx[0] = roll(seam_face, 64, 1)

    def inverse_turn(x):
        total = total_of(mfx[x + 1], mfx[x], mlev[0, x], mlev[1, x])
        inv = inverse_sym([mtens[k, x] for k in range(6)], total)
        for k in range(6):
            mlev[2 + k, x] = inv[k]
        begin = apply_sym(inv, [mlev[8 + c, x] for c in range(3)])
        for c in range(3):
            u1[c, x + 1] = begin[c]

    loop(0, 16, inverse_turn)
    seam(u1)
    bufs = (u1, err)
    for n in range(SWEEPS - 1):
        mid_sweep(bufs[n % 2], bufs[(n + 1) % 2], mfx, mlev)
    count = stage.shape[0] // 4
    stage[...] = jnp.zeros(stage.shape, jnp.float32)

    def rest_turn(a):
        sums = [jnp.zeros(shape, jnp.float32) for _ in range(9 if first else 3)]
        for k in range(4):
            x = a * 4 + k
            fx_up, fx_down = mfx[x + 1], mfx[x]
            fy, fz = mlev[0, x], mlev[1, x]
            total = total_of(fx_up, fx_down, fy, fz)
            here = [err[c, x + 1] for c in range(3)]
            moved = apply_sym([mtens[k, x] for k in range(6)], here)
            for c in range(3):
                sums[c] = sums[c] + (
                    mlev[8 + c, x]
                    + inflow(here[c], err[c, x + 2], err[c, x], fx_up, fx_down, fy, fz)
                    - moved[c]
                    - total * here[c]
                )
            if first:
                for q in range(6):
                    sums[3 + q] = sums[3 + q] + mtens[q, x]
        for q, v in enumerate(sums):
            stage[pl.ds(a * count + q, 1), :] = jnp.sum(v[5:9], axis=0, keepdims=True)

    loop(0, 4, rest_turn)
    for c in range(3):
        for x in range(16):
            v = err[c, x + 1, 5:9]
            to_a[3 + c, x] = v
            to_b[3 + c, x] = v
    square = (128, 128)
    z, to = iota(square, 0), iota(square, 1)
    gather = jnp.where((z // 64 == to // 64) & ((z % 64) // 4 == to % 64), 1.0 / 64.0, 0.0)
    mixed = dot(stage[...], gather)
    value = mixed[0:count]
    for a in range(1, 4):
        value = value + roll(mixed[a * count : (a + 1) * count], 16 * a, 1)
    for s in range(32):
        msg[s] = value


def coarse_kernel(first, *refs):
    if first:
        par, whole, mfx, mlev, err, ea, eb, out, cinv, u0, u1, lifted = refs
    else:
        par, whole, mfx, mlev, err, ea, eb, cinv, out, u0, u1, lifted = refs
    count = whole.shape[0] // 32
    grid = (32, 128)
    row, lane = iota(grid, 0), iota(grid, 1)
    cx, cz = lane // 16, lane % 16
    scale = smooth_weight / 64.0
    one = lambda cond: jnp.where(cond, scale, 0.0)
    ups = (one(cx < 7), one(cx > 0), one(row < 31), one(row > 0), one(cz < 15), one(cz > 0))
    total = ups[0] + ups[1] + ups[2] + ups[3] + ups[4] + ups[5]
    if first:
        inv = inverse_sym([whole[pl.ds(3 + k, 32, stride=count), :] for k in range(6)], total)
        for k in range(6):
            cinv[k] = inv[k]
    inv = [cinv[k] for k in range(6)]
    source = [whole[pl.ds(c, 32, stride=count), :] for c in range(3)]

    def turn(index, now):
        flux = []
        for c in range(3):
            v = now[c]
            flux.append(
                source[c]
                + ups[0] * roll(v, -16, 1)
                + ups[1] * roll(v, 16, 1)
                + ups[2] * roll(v, -1, 0)
                + ups[3] * roll(v, 1, 0)
                + ups[4] * roll(v, -1, 1)
                + ups[5] * roll(v, 1, 1)
            )
        step = apply_sym(inv, flux)
        return tuple((1.0 - damping) * now[c] + step[c] for c in range(3))

    correction = lax.fori_loop(0, COARSE_SWEEPS - 1, turn, tuple(apply_sym(inv, source)))

    shape = (MROWS, 32)
    place = (iota(shape, 0) + (par[1] * 4 - 5)).astype(jnp.float32) * 0.25 - 0.375
    along = hat(place - iota(shape, 1).astype(jnp.float32))
    rows = jnp.concatenate([dot(along, correction[c]) for c in range(3)], axis=0)
    square = (128, 128)
    src, to = iota(square, 0), iota(square, 1)
    depth = hat((to % 64).astype(jnp.float32) * 0.25 - 0.375 - (src % 16).astype(jnp.float32))
    for a in range(4):
        spread = jnp.where(src // 16 == a + 4 * (to // 64), depth, 0.0)
        lifted[a + 1] = dot(rows, spread)
    halves = iota((3 * MROWS, 128), 1) < 64
    lifted[0] = jnp.where(halves, 0.0, roll(lifted[4], 64, 1))
    lifted[5] = jnp.where(halves, roll(lifted[1], 64, 1), 0.0)

    low_of, high_of = sides(par, 1, (4, 128))
    zero = jnp.zeros((MROWS, 128), jnp.float32)
    for x in range(16):
        a, d = x // 4, x % 4
        t = (d + 0.5) / 4 - 0.5
        other = a if t < 0 else a + 2
        added = (1.0 - abs(t)) * lifted[a + 1] + abs(t) * lifted[other]
        for c in range(3):
            u0[c, x + 1] = zero
            u0[c, x + 1, 1:5] = low_of(ea[3 + c, x], eb[3 + c, x])
            u0[c, x + 1, 5:9] = err[c, x + 1, 5:9]
            u0[c, x + 1, 9:13] = high_of(ea[3 + c, x], eb[3 + c, x])
            u0[c, x + 1] = u0[c, x + 1] + added[c * MROWS : (c + 1) * MROWS]
    seam(u0)
    bufs = (u0, u1)
    for n in range(SWEEPS):
        mid_sweep(bufs[n % 2], bufs[(n + 1) % 2], mfx, mlev)

    left = iota((4, 128), 1) < 64
    for b in range(3):
        block = par[0] + (b - 1)
        there = jnp.where((block >= 0) & (block < 8), 1.0, 0.0)
        block = jnp.clip(block, 0, 7)
        upper = (jnp.zeros((4, 128), jnp.int32) + block // 4) == 1
        for k in range(4):
            x = (block % 4) * 4 + k + 1
            v = [u0[c, x, 5:9] for c in range(3)]
            v = [(a, roll(a, 64, 1)) for a in v]
            to_left = [jnp.where(upper, turned, a) for a, turned in v]
            to_right = [jnp.where(upper, a, turned) for a, turned in v]
            out[0, b * 4 + k] = jnp.where(left, to_left[0], to_right[1]) * there
            out[1, b * 4 + k] = jnp.where(left, to_left[2], 0.0) * there


def post_kernel(par, flow, fa, fb, ya, yb, mine, ea, eb, lev, tens, out, u0, u1, mixed, lifted, tall):
    low_of, high_of = sides(par, 1, (4, 128))
    zero = jnp.zeros((4, 128), jnp.float32)

    def place(c, k, v):
        u0[c, 2 + k, 8:16] = v

    wide_layers(par, flow, fa, fb, place)

    def edge_turn(k):
        for c in range(3):
            u0[c, 2 + k, 0:4] = zero
            u0[c, 2 + k, 4:8] = low_of(ya[c, k], yb[c, k])
            u0[c, 2 + k, 16:20] = high_of(ya[c, k], yb[c, k])
            u0[c, 2 + k, 20:24] = zero

    loop(0, 16, edge_turn)
    for x in range(12):
        for p in range(2):
            v = [low_of(ea[p, x], eb[p, x]), mine[p, x], high_of(ea[p, x], eb[p, x])]
            for q in range(3):
                mixed[2 * p, x, 4 * q : 4 * q + 4] = v[q]
            mixed[2 * p, x, 12:16] = zero
    square = (128, 128)
    src, to = iota(square, 0), iota(square, 1)
    place = to.astype(jnp.float32) * 0.5 - 0.25
    depth = hat(place - (src % 64).astype(jnp.float32))
    low = jnp.where(src < 64, depth, 0.0)
    high = jnp.where(src < 64, 0.0, depth)
    for c in range(3):
        v = mixed[2 * (c // 2)].reshape(12 * 16, 128)
        lifted[c] = dot(v, high if c == 1 else low).reshape(12, 16, 128)

    def tall_turn(x):
        for c in range(3):
            v = lifted[c, x]
            tall[c, x, pl.ds(0, 12, stride=2), :] = (0.75 * v + 0.25 * roll(v, 1, 0))[0:12]
            tall[c, x, pl.ds(1, 12, stride=2), :] = (0.75 * v + 0.25 * roll(v, -1, 0))[0:12]

    loop(0, 12, tall_turn)

    def add_turn(m):
        for c in range(3):
            a, b, d = tall[c, m - 1], tall[c, m], tall[c, m + 1]
            x = 2 * m - 2
            u0[c, x] = u0[c, x] + (0.75 * b + 0.25 * a)
            u0[c, x + 1] = u0[c, x + 1] + (0.75 * b + 0.25 * d)

    loop(2, 10, add_turn)
    bufs = (u0, u1)
    for n in range(SWEEPS):
        fine_sweep(bufs[n % 2], bufs[(n + 1) % 2], 3 + n, 17 - n, lev, tens)
    for c in range(3):
        for k in range(8):
            out[c, k] = u0[c, 6 + k, 8:16]


def f32(*shape):
    return jax.ShapeDtypeStruct(shape, jnp.float32)


def call(kernel, outs, scratch, args):
    specs = [pl.BlockSpec(memory_space=pltpu.SMEM)]
    specs += [pl.BlockSpec(memory_space=pltpu.VMEM)] * (len(args) - 1)
    return pl.pallas_call(
        kernel,
        in_specs=specs,
        out_specs=[pl.BlockSpec(memory_space=pltpu.VMEM)] * len(outs),
        out_shape=[f32(*shape) for shape in outs],
        scratch_shapes=[pltpu.VMEM(shape, jnp.float32) for shape in scratch],
        compiler_params=pltpu.CompilerParams(vmem_limit_bytes=20 * 2**20),
        cost_estimate=pl.CostEstimate(flops=20_000_000, bytes_accessed=1_000_000, transcendentals=0),
    )(*args)


def pairs_of(size, start):
    pairs = []
    for k in range(start, size - 1, 2):
        pairs += [(k, k + 1), (k + 1, k)]
    return pairs


def across(field, axes, start):
    return lax.ppermute(field, axes, pairs_of(lax.axis_size(axes), start))


def beside(field, axes):
    return [across(field, axes, 0), across(field, axes, 1)]


def shared(message, axes):
    return lax.all_to_all(message, axes, 0, 0, tiled=True)


def body(first_image, second_image, start_flow):
    par = jnp.stack([lax.axis_index(GX), lax.axis_index(GY)]).astype(jnp.int32)
    block = jnp.concatenate([start_flow, first_image[None], second_image[None]])
    flow = start_flow
    tens = mtens = cinv = None
    fine_shape, mid_shape = (WIDE, ROWS, 128), (16, MROWS, 128)
    for cycle in range(CYCLES):
        first = cycle == 0
        sent = block if first else flow
        fields = sent.shape[0]
        args = [par, sent, *beside(sent, GX)]
        (wide,) = call(functools.partial(widen_kernel, 6), [(fields, WIDE, 8, 128)], [], args)
        size = 88 if first else 40
        stage = (6 if first else 3) * 32
        outs = [(3, 8, 8, 128), (8, size, 128), (9, *fine_shape)]
        scratch = [(fields, *fine_shape), (3, *fine_shape), fine_shape, (stage, 128), (stage, 128), (stage, 128)]
        args = [par, wide, *beside(wide, GY)]
        pre = functools.partial(pre_kernel, first)
        if first:
            flow, message, lev, tens = call(pre, [*outs, (9, *fine_shape)], scratch, args)
        else:
            flow, message, lev = call(pre, outs, scratch, [*args, tens])
        layers = beside(flow, GX)
        mids = shared(message, GX)
        args = [par, mids, *beside(mids, GY), flow, *layers]
        count = 16 if first else 8
        sides_shape = (6, 16, 4, 128)
        outs = [(32, count, 128), sides_shape, sides_shape, (17, MROWS, 128), (11, *mid_shape), (3, 18, MROWS, 128)]
        scratch = [(3, 18, MROWS, 128), mid_shape, (4 * count, 128)]
        mid = functools.partial(mid_kernel, first)
        if first:
            coarse, to_a, to_b, mfx, mlev, err, mtens = call(mid, [*outs, (6, *mid_shape)], scratch, args)
        else:
            coarse, to_a, to_b, mfx, mlev, err = call(mid, outs, scratch, [*args, mtens])
        edges = [across(to_a, GY, 0), across(to_b, GY, 1)]
        whole = shared(coarse, GY).reshape(32 * count, 128)
        args = [par, whole, mfx, mlev, err, *edges]
        outs = [(2, 12, 4, 128)]
        scratch = [(3, 18, MROWS, 128), (3, 18, MROWS, 128), (6, 3 * MROWS, 128)]
        low = functools.partial(coarse_kernel, first)
        if first:
            error, cinv = call(low, [*outs, (6, 32, 128)], scratch, args)
        else:
            (error,) = call(low, outs, scratch, [*args, cinv])
        args = [par, flow, *layers, *edges, error, *beside(error, GY), lev, tens]
        scratch = [(3, *fine_shape), (3, *fine_shape), (3, 12, 16, 128), (3, 12, 16, 128), (3, 12, 24, 128)]
        (flow,) = call(post_kernel, [(3, 8, 8, 128)], scratch, args)
    return flow


def solution(mesh):
    finer = Mesh(mesh.devices.reshape(4, 2, 8, 4), ("gx_0", "gx_1", "gy_0", "gy_1"))
    return jax.shard_map(
        body,
        mesh=finer,
        in_specs=(P(GX, GY, None), P(GX, GY, None), P(None, GX, GY, None)),
        out_specs=P(None, GX, GY, None),
        check_vma=False,
    )
```

```python
import functools

import jax
import jax.numpy as jnp
from jax import lax
from jax.experimental import pallas as pl
from jax.experimental.pallas import tpu as pltpu
from jax.sharding import Mesh
from jax.sharding import PartitionSpec as P


SWEEPS = 4
COARSE_SWEEPS = 12
CYCLES = 2
GX = ("gx_0", "gx_1")
GY = ("gy_0", "gy_1")

damping = 0.6
smooth_weight = 2.0
floor_grad = 0.5

NX, NY = 64, 256
ROWS = 24
WIDE = 20
MROWS = 16


def roll(v, shift, axis):
    return pltpu.roll(v, shift % v.shape[axis], axis)


def iota(shape, dim):
    return lax.broadcasted_iota(jnp.int32, shape, dim)


def face(a, b, scale):
    summed = a + b
    return (2.0 * scale) * a * b / jnp.where(summed > 0.0, summed, 1.0)


def inverse_sym(tensor, total):
    aaa = tensor[0] + total
    bbb = tensor[1]
    ccc = tensor[2]
    ddd = tensor[3] + total
    eee = tensor[4]
    fff = tensor[5] + total
    cof_a = ddd * fff - eee * eee
    cof_b = ccc * eee - bbb * fff
    cof_c = bbb * eee - ccc * ddd
    cof_d = aaa * fff - ccc * ccc
    cof_e = bbb * ccc - aaa * eee
    cof_f = aaa * ddd - bbb * bbb
    determinant = aaa * cof_a + bbb * cof_b + ccc * cof_c
    share = jnp.where(total > 0.0, damping / determinant, 0.0)
    return [cof * share for cof in (cof_a, cof_b, cof_c, cof_d, cof_e, cof_f)]


def apply_sym(m, v):
    return [
        m[0] * v[0] + m[1] * v[1] + m[2] * v[2],
        m[1] * v[0] + m[3] * v[1] + m[4] * v[2],
        m[2] * v[0] + m[4] * v[1] + m[5] * v[2],
    ]


def inflow(here, above, below, fx_up, fx_down, fy, fz):
    return (
        fx_up * above
        + fx_down * below
        + fy * roll(here, -1, 0)
        + roll(fy * here, 1, 0)
        + fz * roll(here, -1, 1)
        + roll(fz * here, 1, 1)
    )


def total_of(fx_up, fx_down, fy, fz):
    return fx_up + fx_down + fy + roll(fy, 1, 0) + fz + roll(fz, 1, 1)


def loop(low, high, turn):
    for index in range(low, high):
        turn(index)


def moved(pairs, sems):
    copies = [pltpu.make_async_copy(a, b, sems.at[k]) for k, (a, b) in enumerate(pairs)]
    for copy in copies:
        copy.start()
    return copies


def sides(par, which, shape):
    is_odd = (jnp.zeros(shape, jnp.int32) + (par[which] & 1)) == 1
    return (lambda a, b: jnp.where(is_odd, a, b)), (lambda a, b: jnp.where(is_odd, b, a))


def hat(distance):
    return jnp.maximum(1.0 - jnp.abs(distance), 0.0)


def dot(a, b):
    return jnp.dot(a, b, precision=lax.Precision.HIGHEST, preferred_element_type=jnp.float32)


def fine_sweep(source, target, low, high, lev, tens):
    def turn(x):
        fx_up, fx_down = lev[0, x], lev[0, x - 1]
        fy, fz = lev[1, x], lev[2, x]
        here = [source[c, x] for c in range(3)]
        flux = [
            tens[6 + c, x]
            + inflow(here[c], source[c, x + 1], source[c, x - 1], fx_up, fx_down, fy, fz)
            for c in range(3)
        ]
        step = apply_sym([lev[3 + k, x] for k in range(6)], flux)
        for c in range(3):
            target[c, x] = (1.0 - damping) * here[c] + step[c]

    loop(low, high, turn)


def widen_kernel(layers, par, own, xa, xb, out):
    shape = (8, 128)
    low_of, high_of = sides(par, 0, shape)
    for f in range(own.shape[0]):
        for k in range(layers):
            out[f, k] = low_of(xa[f, 8 - layers + k], xb[f, 8 - layers + k])
            out[f, layers + 8 + k] = high_of(xa[f, k], xb[f, k])
        for k in range(8):
            out[f, layers + k] = own[f, k]


def stack_rows(par, own, ya, yb, out, fields):
    low_of, high_of = sides(par, 1, (8, 128))

    def turn(x):
        for f in range(fields):
            a, b = ya[f, x], yb[f, x]
            out[f, x, 0:8] = low_of(a, b)
            out[f, x, 8:16] = own[f, x]
            out[f, x, 16:24] = high_of(a, b)

    loop(0, own.shape[1], turn)


def pre_kernel(first, *refs):
    if first:
        par, own, ya, yb, flow_out, msg, lev_far, tens_far, lev, tens, u0, u1, w, even, odd, sums, sems = refs
    else:
        par, own, ya, yb, tens_far, flow_out, msg, lev_far, lev, tens, u0, u1, w, even, odd, sums, sems = refs
        (tens_copy,) = moved([(tens_far, tens)], sems)
    shape = (ROWS, 128)
    lane = iota(shape, 1)
    last, start = lane == 127, lane == 0
    stack_rows(par, own, ya, yb, u0, own.shape[0])

    def z_slope(v):
        return jnp.where(last, 0.0, roll(v, -1, 1)) - jnp.where(start, 0.0, roll(v, 1, 1))

    def y_slope(v):
        return roll(v, -1, 0) - roll(v, 1, 0)

    if first:

        def tensor_turn(x):
            mean = 0.5 * (u0[3, x] + u0[4, x])
            sx = 0.25 * ((u0[3, x + 1] + u0[4, x + 1]) - (u0[3, x - 1] + u0[4, x - 1]))
            sy = 0.5 * y_slope(mean)
            sz = 0.5 * z_slope(mean)
            change = u0[4, x] - u0[3, x]
            scale = 1.0 / (sx * sx + sy * sy + sz * sz + floor_grad)
            gx, gy, gz = scale * sx, scale * sy, scale * sz
            for k, v in enumerate((gx * sx, gx * sy, gx * sz, gy * sy, gy * sz, gz * sz)):
                tens[k, x] = v
            for k, v in enumerate((gx, gy, gz)):
                tens[6 + k, x] = -v * change

        loop(2, 18, tensor_turn)

    row = iota(shape, 0) + (par[1] * 8 - 8)
    inside_y = (row >= 0) & (row < NY)

    def weight_turn(x):
        total = jnp.ones(shape, jnp.float32)
        for c in range(3):
            v = u0[c, x]
            for slope in (u0[c, x + 1] - u0[c, x - 1], y_slope(v), z_slope(v)):
                total = total + slope * slope
        place = x + (par[0] * 8 - 6)
        keep = jnp.where((place >= 0) & (place < NX), 1.0, 0.0)
        w[x] = jnp.where(inside_y, lax.rsqrt(total), 0.0) * keep

    loop(1, 19, weight_turn)

    def face_turn(x):
        v = w[x]
        lev[0, x] = face(v, w[x + 1], smooth_weight)
        lev[1, x] = face(v, roll(v, -1, 0), smooth_weight)
        lev[2, x] = jnp.where(last, 0.0, face(v, roll(v, -1, 1), smooth_weight))

    loop(1, 18, face_turn)

    if not first:
        tens_copy.wait()

    def inverse_turn(x):
        total = total_of(lev[0, x], lev[0, x - 1], lev[1, x], lev[2, x])
        for k, v in enumerate(inverse_sym([tens[k, x] for k in range(6)], total)):
            lev[3 + k, x] = v

    loop(2, 18, inverse_turn)
    far = [(lev, lev_far), (tens, tens_far)] if first else [(lev, lev_far)]
    copies = moved(far, sems)
    bufs = (u0, u1)
    for n in range(SWEEPS):
        fine_sweep(bufs[n % 2], bufs[(n + 1) % 2], 2 + n, 18 - n, lev, tens)

    def rest_at(x):
        fx_up, fx_down = lev[0, x], lev[0, x - 1]
        fy, fz = lev[1, x], lev[2, x]
        total = total_of(fx_up, fx_down, fy, fz)
        here = [u0[c, x] for c in range(3)]
        moved = apply_sym([tens[k, x] for k in range(6)], here)
        return [
            (
                tens[6 + c, x]
                + inflow(here[c], u0[c, x + 1], u0[c, x - 1], fx_up, fx_down, fy, fz)
                - moved[c]
                - total * here[c]
            )[8:16]
            for c in range(3)
        ]

    def rest_turn(m):
        x = 6 + 2 * m
        rest = [a + b for a, b in zip(rest_at(x), rest_at(x + 1))]
        pair = w[x] + w[x + 1]
        fields = rest + [pair[8:16], roll(pair, 2, 0)[8:16], pair[16:24]]
        if first:
            fields += [tens[k, x, 8:16] + tens[k, x + 1, 8:16] for k in range(6)]
        for k, v in enumerate(fields):
            stage = odd if k % 2 else even
            at = (k // 2) * 32 + m * 8
            stage[at : at + 8] = v

    loop(0, 4, rest_turn)
    for c in range(3):
        for k in range(8):
            flow_out[c, k] = u0[c, 6 + k, 8:16]
    square = (128, 128)
    into = iota(square, 0) // 2
    low = jnp.where(into == iota(square, 1), 0.125, 0.0)
    high = jnp.where(into + 64 == iota(square, 1), 0.125, 0.0)
    sums[...] = dot(even[...], low) + dot(odd[...], high)
    pairs = even.shape[0] // 32
    size = msg.shape[1]
    at = 0
    for p in range(pairs):
        if p == 2:
            v = sums[pl.ds(64, 4, stride=8), :] + sums[pl.ds(65, 4, stride=8), :]
            for s in range(8):
                msg[s, size - 8 : size - 4] = v
                msg[s, size - 4 : size] = v
            continue
        v = sums[pl.ds(p * 32, 16, stride=2), :] + sums[pl.ds(p * 32 + 1, 16, stride=2), :]
        for s in range(8):
            msg[s, at : at + 16] = v
        at += 16
    for copy in copies:
        copy.wait()


def wide_layers(par, own, xa, xb, place):
    low_of, high_of = sides(par, 0, (8, 128))
    for c in range(3):
        for k in range(4):
            place(c, k, low_of(xa[c, 4 + k], xb[c, 4 + k]))
            place(c, 12 + k, high_of(xa[c, k], xb[c, k]))
        for k in range(8):
            place(c, 4 + k, own[c, k])


def send_flow(par, flow, fa, fb, to_a, to_b):
    first_of, second_of = sides(par, 1, (4, 128))

    def place(c, k, v):
        to_a[c, k] = first_of(v[0:4], v[4:8])
        to_b[c, k] = second_of(v[0:4], v[4:8])

    wide_layers(par, flow, fa, fb, place)


def mid_sweep(source, target, mfx, mlev):
    def turn(x):
        fx_up, fx_down = mfx[x + 1], mfx[x]
        fy, fz = mlev[0, x], mlev[1, x]
        here = [source[c, x + 1] for c in range(3)]
        flux = [
            mlev[8 + c, x]
            + inflow(here[c], source[c, x + 2], source[c, x], fx_up, fx_down, fy, fz)
            for c in range(3)
        ]
        step = apply_sym([mlev[2 + k, x] for k in range(6)], flux)
        for c in range(3):
            target[c, x + 1] = (1.0 - damping) * here[c] + step[c]

    loop(0, 16, turn)
    seam(target)


def seam(field):
    for c in range(3):
        field[c, 0] = roll(field[c, 16], 64, 1)
        field[c, 17] = roll(field[c, 1], 64, 1)


def mid_kernel(first, *refs):
    if first:
        par, own, ya, yb, flow, fa, fb, msg, to_a, to_b, *refs = refs
        mfx_far, mlev_far, err_far, mtens_far, mfx, mlev, err, mtens, u1, w, stage, sems = refs
    else:
        par, own, ya, yb, flow, fa, fb, mtens_far, msg, to_a, to_b, *refs = refs
        mfx_far, mlev_far, err_far, mfx, mlev, err, mtens, u1, w, stage, sems = refs
        (mtens_copy,) = moved([(mtens_far, mtens)], sems)
    send_flow(par, flow, fa, fb, to_a, to_b)
    shape = (MROWS, 128)
    lane = iota(shape, 1)
    left = iota((8, 128), 1) < 64
    low_of, high_of = sides(par, 1, (8, 128))
    size = own.shape[1]
    zero4 = jnp.zeros((4, 128), jnp.float32)

    def split(a, b, which):
        if which:
            return jnp.where(left, roll(a, 64, 1), b)
        return jnp.where(left, a, roll(b, 64, 1))

    def fields_of(out, slot, pair, which):
        def turn(a):
            for kk in range(2):
                rows = slice(pair * 16 + kk * 8, pair * 16 + kk * 8 + 8)
                la, lb = low_of(ya[a, rows], yb[a, rows]), low_of(ya[a + 4, rows], yb[a + 4, rows])
                ha, hb = high_of(ya[a, rows], yb[a, rows]), high_of(ya[a + 4, rows], yb[a + 4, rows])
                for base, va, vb in ((1, la, lb), (5, own[a, rows], own[a + 4, rows]), (9, ha, hb)):
                    v = split(va, vb, which)
                    for k in range(2):
                        x = a * 4 + kk * 2 + k
                        if slot is None:
                            out[x, base : base + 4] = v[4 * k : 4 * k + 4]
                        else:
                            out[slot, x, base : base + 4] = v[4 * k : 4 * k + 4]

        loop(0, 4, turn)

    def clear_turn(x):
        for ref in (w,):
            ref[x, 0:1] = zero4[0:1]
            ref[x, 13:16] = zero4[0:3]
        for k in range(3):
            mlev[8 + k, x, 0:1] = zero4[0:1]
            mlev[8 + k, x, 13:16] = zero4[0:3]
        if first:
            for k in range(6):
                mtens[k, x, 0:1] = zero4[0:1]
                mtens[k, x, 13:16] = zero4[0:3]

    loop(0, 16, clear_turn)
    fields_of(mlev, 8, 0, 0)
    fields_of(mlev, 9, 0, 1)
    fields_of(mlev, 10, 1, 0)
    fields_of(w, None, 1, 1)
    if first:
        for k in range(6):
            fields_of(mtens, k, 2 + k // 2, k % 2)
    outer = slice(size - 8, size)
    for a in range(4):
        la, lb = low_of(ya[a, outer], yb[a, outer]), low_of(ya[a + 4, outer], yb[a + 4, outer])
        ha, hb = high_of(ya[a, outer], yb[a, outer]), high_of(ya[a + 4, outer], yb[a + 4, outer])
        lo, hi = split(la, lb, 0), split(ha, hb, 1)
        for k in range(4):
            w[a * 4 + k, 0:1] = lo[k : k + 1]
            w[a * 4 + k, 13:14] = hi[k : k + 1]

    scale = smooth_weight / 4.0
    stop = (lane == 63) | (lane == 127)

    def face_turn(x):
        v = w[x]
        mlev[0, x] = face(v, roll(v, -1, 0), scale)
        mlev[1, x] = jnp.where(stop, 0.0, face(v, roll(v, -1, 1), scale))

    loop(0, 16, face_turn)

    def across_turn(x):
        mfx[x + 1] = face(w[x], w[x + 1], scale)

    loop(0, 15, across_turn)
    seam_face = jnp.where(lane < 64, face(w[15], roll(w[0], 64, 1), scale), 0.0)
    mfx[16] = seam_face
    mfx[0] = roll(seam_face, 64, 1)

    if not first:
        mtens_copy.wait()

    def inverse_turn(x):
        total = total_of(mfx[x + 1], mfx[x], mlev[0, x], mlev[1, x])
        inv = inverse_sym([mtens[k, x] for k in range(6)], total)
        for k in range(6):
            mlev[2 + k, x] = inv[k]
        begin = apply_sym(inv, [mlev[8 + c, x] for c in range(3)])
        for c in range(3):
            u1[c, x + 1] = begin[c]

    loop(0, 16, inverse_turn)
    seam(u1)
    far = [(mfx, mfx_far), (mlev, mlev_far)]
    copies = moved(far + [(mtens, mtens_far)] if first else far, sems)
    bufs = (u1, err)
    for n in range(SWEEPS - 1):
        mid_sweep(bufs[n % 2], bufs[(n + 1) % 2], mfx, mlev)
    (err_copy,) = moved([(err, err_far)], sems.at[3:4])
    count = stage.shape[0] // 4
    stage[...] = jnp.zeros(stage.shape, jnp.float32)

    def rest_turn(a):
        sums = [jnp.zeros(shape, jnp.float32) for _ in range(9 if first else 3)]
        for k in range(4):
            x = a * 4 + k
            fx_up, fx_down = mfx[x + 1], mfx[x]
            fy, fz = mlev[0, x], mlev[1, x]
            total = total_of(fx_up, fx_down, fy, fz)
            here = [err[c, x + 1] for c in range(3)]
            moved = apply_sym([mtens[k, x] for k in range(6)], here)
            for c in range(3):
                sums[c] = sums[c] + (
                    mlev[8 + c, x]
                    + inflow(here[c], err[c, x + 2], err[c, x], fx_up, fx_down, fy, fz)
                    - moved[c]
                    - total * here[c]
                )
            if first:
                for q in range(6):
                    sums[3 + q] = sums[3 + q] + mtens[q, x]
        for q, v in enumerate(sums):
            stage[a * count + q : a * count + q + 1] = jnp.sum(v[5:9], axis=0, keepdims=True)

    loop(0, 4, rest_turn)
    for c in range(3):
        for x in range(16):
            v = err[c, x + 1, 5:9]
            to_a[3 + c, x] = v
            to_b[3 + c, x] = v
    square = (128, 128)
    z, to = iota(square, 0), iota(square, 1)
    gather = jnp.where((z // 64 == to // 64) & ((z % 64) // 4 == to % 64), 1.0 / 64.0, 0.0)
    mixed = dot(stage[...], gather)
    value = mixed[0:count]
    for a in range(1, 4):
        value = value + roll(mixed[a * count : (a + 1) * count], 16 * a, 1)
    for s in range(32):
        msg[s] = value
    for copy in [*copies, err_copy]:
        copy.wait()


def coarse_kernel(first, *refs):
    if first:
        par, whole, mfx_far, mlev_far, err_far, ea, eb, out, cinv_far, mfx, mlev, err, cinv, u0, u1, lifted, sems = refs
    else:
        par, whole, mfx_far, mlev_far, err_far, ea, eb, cinv, out, mfx, mlev, err, u0, u1, lifted, sems = refs
    copies = moved([(mfx_far, mfx), (mlev_far, mlev), (err_far, err)], sems)
    count = whole.shape[0] // 32
    grid = (32, 128)
    row, lane = iota(grid, 0), iota(grid, 1)
    cx, cz = lane // 16, lane % 16
    scale = smooth_weight / 64.0
    one = lambda cond: jnp.where(cond, scale, 0.0)
    ups = (one(cx < 7), one(cx > 0), one(row < 31), one(row > 0), one(cz < 15), one(cz > 0))
    total = ups[0] + ups[1] + ups[2] + ups[3] + ups[4] + ups[5]
    if first:
        inv = inverse_sym([whole[pl.ds(3 + k, 32, stride=count), :] for k in range(6)], total)
        for k in range(6):
            cinv[k] = inv[k]
        copies += moved([(cinv, cinv_far)], sems.at[3:4])
    inv = [cinv[k] for k in range(6)]
    source = [whole[pl.ds(c, 32, stride=count), :] for c in range(3)]

    def turn(index, now):
        flux = []
        for c in range(3):
            v = now[c]
            flux.append(
                source[c]
                + ups[0] * roll(v, -16, 1)
                + ups[1] * roll(v, 16, 1)
                + ups[2] * roll(v, -1, 0)
                + ups[3] * roll(v, 1, 0)
                + ups[4] * roll(v, -1, 1)
                + ups[5] * roll(v, 1, 1)
            )
        step = apply_sym(inv, flux)
        return tuple((1.0 - damping) * now[c] + step[c] for c in range(3))

    correction = lax.fori_loop(0, COARSE_SWEEPS - 1, turn, tuple(apply_sym(inv, source)))

    shape = (MROWS, 32)
    place = (iota(shape, 0) + (par[1] * 4 - 5)).astype(jnp.float32) * 0.25 - 0.375
    along = hat(place - iota(shape, 1).astype(jnp.float32))
    rows = jnp.concatenate([dot(along, correction[c]) for c in range(3)], axis=0)
    square = (128, 128)
    src, to = iota(square, 0), iota(square, 1)
    depth = hat((to % 64).astype(jnp.float32) * 0.25 - 0.375 - (src % 16).astype(jnp.float32))
    for a in range(4):
        spread = jnp.where(src // 16 == a + 4 * (to // 64), depth, 0.0)
        lifted[a + 1] = dot(rows, spread)
    halves = iota((3 * MROWS, 128), 1) < 64
    lifted[0] = jnp.where(halves, 0.0, roll(lifted[4], 64, 1))
    lifted[5] = jnp.where(halves, roll(lifted[1], 64, 1), 0.0)

    for copy in copies:
        copy.wait()
    low_of, high_of = sides(par, 1, (4, 128))
    zero = jnp.zeros((MROWS, 128), jnp.float32)
    for x in range(16):
        a, d = x // 4, x % 4
        t = (d + 0.5) / 4 - 0.5
        other = a if t < 0 else a + 2
        added = (1.0 - abs(t)) * lifted[a + 1] + abs(t) * lifted[other]
        for c in range(3):
            u0[c, x + 1] = zero
            u0[c, x + 1, 1:5] = low_of(ea[3 + c, x], eb[3 + c, x])
            u0[c, x + 1, 5:9] = err[c, x + 1, 5:9]
            u0[c, x + 1, 9:13] = high_of(ea[3 + c, x], eb[3 + c, x])
            u0[c, x + 1] = u0[c, x + 1] + added[c * MROWS : (c + 1) * MROWS]
    seam(u0)
    bufs = (u0, u1)
    for n in range(SWEEPS):
        mid_sweep(bufs[n % 2], bufs[(n + 1) % 2], mfx, mlev)

    left = iota((4, 128), 1) < 64
    for b in range(3):
        block = par[0] + (b - 1)
        there = jnp.where((block >= 0) & (block < 8), 1.0, 0.0)
        block = jnp.clip(block, 0, 7)
        upper = (jnp.zeros((4, 128), jnp.int32) + block // 4) == 1
        for k in range(4):
            x = (block % 4) * 4 + k + 1
            v = [u0[c, x, 5:9] for c in range(3)]
            v = [(a, roll(a, 64, 1)) for a in v]
            to_left = [jnp.where(upper, turned, a) for a, turned in v]
            to_right = [jnp.where(upper, a, turned) for a, turned in v]
            out[0, b * 4 + k] = jnp.where(left, to_left[0], to_right[1]) * there
            out[1, b * 4 + k] = jnp.where(left, to_left[2], 0.0) * there


def post_kernel(par, flow, fa, fb, ya, yb, mine, ea, eb, lev_far, tens_far, out, lev, tens, u0, u1, mixed, lifted, tall, sems):
    copies = moved([(lev_far, lev), (tens_far.at[6:9], tens.at[6:9])], sems)
    low_of, high_of = sides(par, 1, (4, 128))
    zero = jnp.zeros((4, 128), jnp.float32)

    def place(c, k, v):
        u0[c, 2 + k, 8:16] = v

    wide_layers(par, flow, fa, fb, place)

    def edge_turn(k):
        for c in range(3):
            u0[c, 2 + k, 0:4] = zero
            u0[c, 2 + k, 4:8] = low_of(ya[c, k], yb[c, k])
            u0[c, 2 + k, 16:20] = high_of(ya[c, k], yb[c, k])
            u0[c, 2 + k, 20:24] = zero

    loop(0, 16, edge_turn)
    for x in range(12):
        for p in range(2):
            v = [low_of(ea[p, x], eb[p, x]), mine[p, x], high_of(ea[p, x], eb[p, x])]
            for q in range(3):
                mixed[2 * p, x, 4 * q : 4 * q + 4] = v[q]
            mixed[2 * p, x, 12:16] = zero
    square = (128, 128)
    src, to = iota(square, 0), iota(square, 1)
    place = to.astype(jnp.float32) * 0.5 - 0.25
    depth = hat(place - (src % 64).astype(jnp.float32))
    low = jnp.where(src < 64, depth, 0.0)
    high = jnp.where(src < 64, 0.0, depth)
    for c in range(3):
        v = mixed[2 * (c // 2)].reshape(12 * 16, 128)
        lifted[c] = dot(v, high if c == 1 else low).reshape(12, 16, 128)

    def tall_turn(x):
        for c in range(3):
            v = lifted[c, x]
            tall[c, x, pl.ds(0, 12, stride=2), :] = (0.75 * v + 0.25 * roll(v, 1, 0))[0:12]
            tall[c, x, pl.ds(1, 12, stride=2), :] = (0.75 * v + 0.25 * roll(v, -1, 0))[0:12]

    loop(0, 12, tall_turn)

    def add_turn(m):
        for c in range(3):
            a, b, d = tall[c, m - 1], tall[c, m], tall[c, m + 1]
            x = 2 * m - 2
            u0[c, x] = u0[c, x] + (0.75 * b + 0.25 * a)
            u0[c, x + 1] = u0[c, x + 1] + (0.75 * b + 0.25 * d)

    loop(2, 10, add_turn)
    for copy in copies:
        copy.wait()
    bufs = (u0, u1)
    for n in range(SWEEPS):
        fine_sweep(bufs[n % 2], bufs[(n + 1) % 2], 3 + n, 17 - n, lev, tens)
    for c in range(3):
        for k in range(8):
            out[c, k] = u0[c, 6 + k, 8:16]


def f32(*shape):
    return jax.ShapeDtypeStruct(shape, jnp.float32)


def call(kernel, outs, scratch, args, far_in=(), far_out=(), sems=0):
    near, far = pl.BlockSpec(memory_space=pltpu.VMEM), pl.BlockSpec(memory_space=pltpu.HBM)
    args = [pltpu.with_memory_space_constraint(v, pltpu.HBM) if k in far_in else v for k, v in enumerate(args)]
    specs = [pl.BlockSpec(memory_space=pltpu.SMEM)]
    specs += [far if k in far_in else near for k in range(1, len(args))]
    scratch_shapes = [pltpu.VMEM(shape, jnp.float32) for shape in scratch]
    if sems:
        scratch_shapes.append(pltpu.SemaphoreType.DMA((sems,)))
    return pl.pallas_call(
        kernel,
        in_specs=specs,
        out_specs=[far if k in far_out else near for k in range(len(outs))],
        out_shape=[pltpu.HBM(shape, jnp.float32) if k in far_out else f32(*shape) for k, shape in enumerate(outs)],
        scratch_shapes=scratch_shapes,
        compiler_params=pltpu.CompilerParams(vmem_limit_bytes=24 * 2**20),
        cost_estimate=pl.CostEstimate(flops=20_000_000, bytes_accessed=1_000_000, transcendentals=0),
    )(*args)


def pairs_of(size, start):
    pairs = []
    for k in range(start, size - 1, 2):
        pairs += [(k, k + 1), (k + 1, k)]
    return pairs


def across(field, axes, start):
    return lax.ppermute(field, axes, pairs_of(lax.axis_size(axes), start))


def beside(field, axes):
    return [across(field, axes, 0), across(field, axes, 1)]


def shared(message, axes):
    return lax.all_to_all(message, axes, 0, 0, tiled=True)


def body(first_image, second_image, start_flow):
    par = jnp.stack([lax.axis_index(GX), lax.axis_index(GY)]).astype(jnp.int32)
    block = jnp.concatenate([start_flow, first_image[None], second_image[None]])
    flow = start_flow
    tens = mtens = cinv = None
    fine_shape, mid_shape = (WIDE, ROWS, 128), (16, MROWS, 128)
    for cycle in range(CYCLES):
        first = cycle == 0
        sent = block if first else flow
        fields = sent.shape[0]
        args = [par, sent, *beside(sent, GX)]
        (wide,) = call(functools.partial(widen_kernel, 6), [(fields, WIDE, 8, 128)], [], args)
        size = 88 if first else 40
        stage = (6 if first else 3) * 32
        outs = [(3, 8, 8, 128), (8, size, 128), (9, *fine_shape)]
        scratch = [(9, *fine_shape), (9, *fine_shape), (fields, *fine_shape), (3, *fine_shape), fine_shape]
        scratch += [(stage, 128)] * 3
        args = [par, wide, *beside(wide, GY)]
        pre = functools.partial(pre_kernel, first)
        if first:
            flow, message, lev, tens = call(pre, [*outs, (9, *fine_shape)], scratch, args, (), (2, 3), 2)
        else:
            flow, message, lev = call(pre, outs, scratch, [*args, tens], (4,), (2,), 2)
        layers = beside(flow, GX)
        mids = shared(message, GX)
        args = [par, mids, *beside(mids, GY), flow, *layers]
        count = 16 if first else 8
        sides_shape = (6, 16, 4, 128)
        saved = [(17, MROWS, 128), (11, *mid_shape), (3, 18, MROWS, 128)]
        outs = [(32, count, 128), sides_shape, sides_shape, *saved]
        scratch = [*saved, (6, *mid_shape), (3, 18, MROWS, 128), mid_shape, (4 * count, 128)]
        mid = functools.partial(mid_kernel, first)
        if first:
            coarse, to_a, to_b, mfx, mlev, err, mtens = call(
                mid, [*outs, (6, *mid_shape)], scratch, args, (), (3, 4, 5, 6), 4
            )
        else:
            coarse, to_a, to_b, mfx, mlev, err = call(mid, outs, scratch, [*args, mtens], (7,), (3, 4, 5), 4)
        edges = [across(to_a, GY, 0), across(to_b, GY, 1)]
        whole = shared(coarse, GY).reshape(32 * count, 128)
        args = [par, whole, mfx, mlev, err, *edges]
        outs = [(2, 12, 4, 128)]
        scratch = [(3, 18, MROWS, 128), (3, 18, MROWS, 128), (6, 3 * MROWS, 128)]
        inverse = (6, 32, 128)
        low = functools.partial(coarse_kernel, first)
        if first:
            error, cinv = call(low, [*outs, inverse], [*saved, inverse, *scratch], args, (2, 3, 4), (1,), 4)
        else:
            (error,) = call(low, outs, [*saved, *scratch], [*args, cinv], (2, 3, 4), (), 4)
        args = [par, flow, *layers, *edges, error, *beside(error, GY), lev, tens]
        scratch = [(9, *fine_shape), (9, *fine_shape), (3, *fine_shape), (3, *fine_shape)]
        scratch += [(3, 12, 16, 128), (3, 12, 16, 128), (3, 12, 24, 128)]
        (flow,) = call(post_kernel, [(3, 8, 8, 128)], scratch, args, (9, 10), (), 2)
    return flow


def solution(mesh):
    finer = Mesh(mesh.devices.reshape(4, 2, 8, 4), ("gx_0", "gx_1", "gy_0", "gy_1"))
    return jax.shard_map(
        body,
        mesh=finer,
        in_specs=(P(GX, GY, None), P(GX, GY, None), P(None, GX, GY, None)),
        out_specs=P(None, GX, GY, None),
        check_vma=False,
    )
```

```python
import functools

import jax
import jax.numpy as jnp
from jax import lax
from jax.experimental import pallas as pl
from jax.experimental.pallas import tpu as pltpu
from jax.sharding import Mesh
from jax.sharding import PartitionSpec as P


SWEEPS = 4
COARSE_SWEEPS = 12
CYCLES = 2
GX = ("gx_0", "gx_1")
GY = ("gy_0", "gy_1")

damping = 0.6
smooth_weight = 2.0
floor_grad = 0.5

NX, NY = 64, 256
ROWS = 24
WIDE = 20
MROWS = 16


def roll(v, shift, axis):
    return pltpu.roll(v, shift % v.shape[axis], axis)


def iota(shape, dim):
    return lax.broadcasted_iota(jnp.int32, shape, dim)


def face(a, b, scale):
    summed = a + b
    return (2.0 * scale) * a * b / jnp.where(summed > 0.0, summed, 1.0)


def inverse_sym(tensor, total):
    aaa = tensor[0] + total
    bbb = tensor[1]
    ccc = tensor[2]
    ddd = tensor[3] + total
    eee = tensor[4]
    fff = tensor[5] + total
    cof_a = ddd * fff - eee * eee
    cof_b = ccc * eee - bbb * fff
    cof_c = bbb * eee - ccc * ddd
    cof_d = aaa * fff - ccc * ccc
    cof_e = bbb * ccc - aaa * eee
    cof_f = aaa * ddd - bbb * bbb
    determinant = aaa * cof_a + bbb * cof_b + ccc * cof_c
    share = jnp.where(total > 0.0, damping / determinant, 0.0)
    return [cof * share for cof in (cof_a, cof_b, cof_c, cof_d, cof_e, cof_f)]


def apply_sym(m, v):
    return [
        m[0] * v[0] + m[1] * v[1] + m[2] * v[2],
        m[1] * v[0] + m[3] * v[1] + m[4] * v[2],
        m[2] * v[0] + m[4] * v[1] + m[5] * v[2],
    ]


def inflow(here, above, below, fx_up, fx_down, fy, fz):
    return (
        fx_up * above
        + fx_down * below
        + fy * roll(here, -1, 0)
        + roll(fy * here, 1, 0)
        + fz * roll(here, -1, 1)
        + roll(fz * here, 1, 1)
    )


def total_of(fx_up, fx_down, fy, fz):
    return fx_up + fx_down + fy + roll(fy, 1, 0) + fz + roll(fz, 1, 1)


def loop(low, high, turn):
    for index in range(low, high):
        turn(index)


def moved(pairs, sems):
    copies = [pltpu.make_async_copy(a, b, sems.at[k]) for k, (a, b) in enumerate(pairs)]
    for copy in copies:
        copy.start()
    return copies


def sides(par, which, shape):
    is_odd = (jnp.zeros(shape, jnp.int32) + (par[which] & 1)) == 1
    return (lambda a, b: jnp.where(is_odd, a, b)), (lambda a, b: jnp.where(is_odd, b, a))


def hat(distance):
    return jnp.maximum(1.0 - jnp.abs(distance), 0.0)


def dot(a, b):
    return jnp.dot(a, b, precision=lax.Precision.HIGHEST, preferred_element_type=jnp.float32)


def fine_sweep(source, target, low, high, lev, tens):
    def turn(x):
        fx_up, fx_down = lev[0, x], lev[0, x - 1]
        fy, fz = lev[1, x], lev[2, x]
        here = [source[c, x] for c in range(3)]
        flux = [
            tens[6 + c, x]
            + inflow(here[c], source[c, x + 1], source[c, x - 1], fx_up, fx_down, fy, fz)
            for c in range(3)
        ]
        step = apply_sym([lev[3 + k, x] for k in range(6)], flux)
        for c in range(3):
            target[c, x] = (1.0 - damping) * here[c] + step[c]

    loop(low, high, turn)


def widen_kernel(par, own, xa, xb, wide, to_a, to_b):
    low_of, high_of = sides(par, 0, (8, 128))
    first_of, second_of = sides(par, 1, (4, 128))
    for f in range(own.shape[0]):
        for x in range(WIDE):
            if x < 6:
                v = low_of(xa[f, 2 + x], xb[f, 2 + x])
            elif x < 14:
                v = own[f, x - 6]
            else:
                v = high_of(xa[f, x - 14], xb[f, x - 14])
            wide[f, x] = v
            below, above = v[0:4], v[4:8]
            if 1 <= x < 19:
                to_a[f, x - 1] = first_of(below, above)
                to_b[f, x - 1] = second_of(below, above)
            if 5 <= x < 15:
                to_a[f, 13 + x] = first_of(above, below)
                to_b[f, 13 + x] = second_of(above, below)


def stack_rows(par, own, ya, yb, out):
    low_of, high_of = sides(par, 1, (4, 128))
    zero = jnp.zeros((4, 128), jnp.float32)
    for f in range(own.shape[0]):
        for x in range(WIDE):
            out[f, x, 8:16] = own[f, x]
            near = (ya[f, x - 1], yb[f, x - 1]) if 1 <= x < 19 else (zero, zero)
            far = (ya[f, 13 + x], yb[f, 13 + x]) if 5 <= x < 15 else (zero, zero)
            out[f, x, 0:4] = low_of(*far)
            out[f, x, 4:8] = low_of(*near)
            out[f, x, 16:20] = high_of(*near)
            out[f, x, 20:24] = high_of(*far)


def pre_kernel(first, *refs):
    if first:
        par, own, ya, yb, flow_out, msg, lev_far, tens_far, lev, tens, u0, u1, w, even, odd, sums, sems = refs
    else:
        par, own, ya, yb, tens_far, flow_out, msg, lev_far, lev, tens, u0, u1, w, even, odd, sums, sems = refs
        parts = [(tens_far.at[k, 2:18], tens.at[k, 2:18]) for k in (slice(0, 6), slice(6, 9))]
        tens_copy, source_copy = moved(parts, sems)
    shape = (ROWS, 128)
    lane = iota(shape, 1)
    last, start = lane == 127, lane == 0
    stack_rows(par, own, ya, yb, u0)

    def z_slope(v):
        return jnp.where(last, 0.0, roll(v, -1, 1)) - jnp.where(start, 0.0, roll(v, 1, 1))

    def y_slope(v):
        return roll(v, -1, 0) - roll(v, 1, 0)

    if first:

        def tensor_turn(x):
            mean = 0.5 * (u0[3, x] + u0[4, x])
            sx = 0.25 * ((u0[3, x + 1] + u0[4, x + 1]) - (u0[3, x - 1] + u0[4, x - 1]))
            sy = 0.5 * y_slope(mean)
            sz = 0.5 * z_slope(mean)
            change = u0[4, x] - u0[3, x]
            scale = 1.0 / (sx * sx + sy * sy + sz * sz + floor_grad)
            gx, gy, gz = scale * sx, scale * sy, scale * sz
            for k, v in enumerate((gx * sx, gx * sy, gx * sz, gy * sy, gy * sz, gz * sz)):
                tens[k, x] = v
            for k, v in enumerate((gx, gy, gz)):
                tens[6 + k, x] = -v * change

        loop(2, 18, tensor_turn)

    row = iota(shape, 0) + (par[1] * 8 - 8)
    inside_y = (row >= 0) & (row < NY)

    def weight_turn(x):
        total = jnp.ones(shape, jnp.float32)
        for c in range(3):
            v = u0[c, x]
            for slope in (u0[c, x + 1] - u0[c, x - 1], y_slope(v), z_slope(v)):
                total = total + slope * slope
        place = x + (par[0] * 8 - 6)
        keep = jnp.where((place >= 0) & (place < NX), 1.0, 0.0)
        w[x] = jnp.where(inside_y, lax.rsqrt(total), 0.0) * keep

    loop(1, 19, weight_turn)

    def face_turn(x):
        v = w[x]
        lev[0, x] = face(v, w[x + 1], smooth_weight)
        lev[1, x] = face(v, roll(v, -1, 0), smooth_weight)
        lev[2, x] = jnp.where(last, 0.0, face(v, roll(v, -1, 1), smooth_weight))

    loop(1, 18, face_turn)

    if not first:
        tens_copy.wait()

    def inverse_turn(x):
        total = total_of(lev[0, x], lev[0, x - 1], lev[1, x], lev[2, x])
        for k, v in enumerate(inverse_sym([tens[k, x] for k in range(6)], total)):
            lev[3 + k, x] = v

    loop(2, 18, inverse_turn)
    if not first:
        source_copy.wait()
    far = [(lev, lev_far), (tens, tens_far)] if first else [(lev, lev_far)]
    copies = moved(far, sems)
    bufs = (u0, u1)
    for n in range(SWEEPS):
        fine_sweep(bufs[n % 2], bufs[(n + 1) % 2], 2 + n, 18 - n, lev, tens)

    def rest_at(x):
        fx_up, fx_down = lev[0, x], lev[0, x - 1]
        fy, fz = lev[1, x], lev[2, x]
        total = total_of(fx_up, fx_down, fy, fz)
        here = [u0[c, x] for c in range(3)]
        moved = apply_sym([tens[k, x] for k in range(6)], here)
        return [
            (
                tens[6 + c, x]
                + inflow(here[c], u0[c, x + 1], u0[c, x - 1], fx_up, fx_down, fy, fz)
                - moved[c]
                - total * here[c]
            )[8:16]
            for c in range(3)
        ]

    def rest_turn(m):
        x = 6 + 2 * m
        rest = [a + b for a, b in zip(rest_at(x), rest_at(x + 1))]
        pair = w[x] + w[x + 1]
        fields = rest + [pair[8:16], roll(pair, 2, 0)[8:16], pair[16:24]]
        if first:
            fields += [tens[k, x, 8:16] + tens[k, x + 1, 8:16] for k in range(6)]
        for k, v in enumerate(fields):
            stage = odd if k % 2 else even
            at = (k // 2) * 32 + m * 8
            stage[at : at + 8] = v

    loop(0, 4, rest_turn)
    for c in range(3):
        for k in range(8):
            flow_out[c, k] = u0[c, 6 + k, 8:16]
    square = (128, 128)
    into = iota(square, 0) // 2
    low = jnp.where(into == iota(square, 1), 0.125, 0.0)
    high = jnp.where(into + 64 == iota(square, 1), 0.125, 0.0)
    sums[...] = dot(even[...], low) + dot(odd[...], high)
    pairs = even.shape[0] // 32
    size = msg.shape[1]
    at = 0
    for p in range(pairs):
        if p == 2:
            v = sums[pl.ds(64, 4, stride=8), :] + sums[pl.ds(65, 4, stride=8), :]
            for s in range(8):
                msg[s, size - 8 : size - 4] = v
                msg[s, size - 4 : size] = v
            continue
        v = sums[pl.ds(p * 32, 16, stride=2), :] + sums[pl.ds(p * 32 + 1, 16, stride=2), :]
        for s in range(8):
            msg[s, at : at + 16] = v
        at += 16
    for copy in copies:
        copy.wait()


def wide_layers(par, own, xa, xb, place):
    low_of, high_of = sides(par, 0, (8, 128))
    for c in range(3):
        for k in range(4):
            place(c, k, low_of(xa[c, 4 + k], xb[c, 4 + k]))
            place(c, 12 + k, high_of(xa[c, k], xb[c, k]))
        for k in range(8):
            place(c, 4 + k, own[c, k])


def send_flow(par, flow, fa, fb, to_a, to_b):
    first_of, second_of = sides(par, 1, (4, 128))

    def place(c, k, v):
        to_a[c, k] = first_of(v[0:4], v[4:8])
        to_b[c, k] = second_of(v[0:4], v[4:8])

    wide_layers(par, flow, fa, fb, place)


def mid_sweep(source, target, mfx, mlev):
    def turn(x):
        fx_up, fx_down = mfx[x + 1], mfx[x]
        fy, fz = mlev[0, x], mlev[1, x]
        here = [source[c, x + 1] for c in range(3)]
        flux = [
            mlev[8 + c, x]
            + inflow(here[c], source[c, x + 2], source[c, x], fx_up, fx_down, fy, fz)
            for c in range(3)
        ]
        step = apply_sym([mlev[2 + k, x] for k in range(6)], flux)
        for c in range(3):
            target[c, x + 1] = (1.0 - damping) * here[c] + step[c]

    loop(0, 16, turn)
    seam(target)


def seam(field):
    for c in range(3):
        field[c, 0] = roll(field[c, 16], 64, 1)
        field[c, 17] = roll(field[c, 1], 64, 1)


def mid_kernel(first, *refs):
    if first:
        par, own, ya, yb, flow, fa, fb, msg, to_a, to_b, *refs = refs
        mfx_far, mlev_far, err_far, mtens_far, mfx, mlev, err, mtens, u1, w, stage, sems = refs
    else:
        par, own, ya, yb, flow, fa, fb, mtens_far, msg, to_a, to_b, *refs = refs
        mfx_far, mlev_far, err_far, mfx, mlev, err, mtens, u1, w, stage, sems = refs
        (mtens_copy,) = moved([(mtens_far, mtens)], sems)
    send_flow(par, flow, fa, fb, to_a, to_b)
    shape = (MROWS, 128)
    lane = iota(shape, 1)
    left = iota((8, 128), 1) < 64
    low_of, high_of = sides(par, 1, (8, 128))
    size = own.shape[1]
    zero4 = jnp.zeros((4, 128), jnp.float32)

    def split(a, b, which):
        if which:
            return jnp.where(left, roll(a, 64, 1), b)
        return jnp.where(left, a, roll(b, 64, 1))

    def fields_of(out, slot, pair, which):
        def turn(a):
            for kk in range(2):
                rows = slice(pair * 16 + kk * 8, pair * 16 + kk * 8 + 8)
                la, lb = low_of(ya[a, rows], yb[a, rows]), low_of(ya[a + 4, rows], yb[a + 4, rows])
                ha, hb = high_of(ya[a, rows], yb[a, rows]), high_of(ya[a + 4, rows], yb[a + 4, rows])
                for base, va, vb in ((1, la, lb), (5, own[a, rows], own[a + 4, rows]), (9, ha, hb)):
                    v = split(va, vb, which)
                    for k in range(2):
                        x = a * 4 + kk * 2 + k
                        if slot is None:
                            out[x, base : base + 4] = v[4 * k : 4 * k + 4]
                        else:
                            out[slot, x, base : base + 4] = v[4 * k : 4 * k + 4]

        loop(0, 4, turn)

    def clear_turn(x):
        for ref in (w,):
            ref[x, 0:1] = zero4[0:1]
            ref[x, 13:16] = zero4[0:3]
        for k in range(3):
            mlev[8 + k, x, 0:1] = zero4[0:1]
            mlev[8 + k, x, 13:16] = zero4[0:3]
        if first:
            for k in range(6):
                mtens[k, x, 0:1] = zero4[0:1]
                mtens[k, x, 13:16] = zero4[0:3]

    loop(0, 16, clear_turn)
    fields_of(mlev, 8, 0, 0)
    fields_of(mlev, 9, 0, 1)
    fields_of(mlev, 10, 1, 0)
    fields_of(w, None, 1, 1)
    if first:
        for k in range(6):
            fields_of(mtens, k, 2 + k // 2, k % 2)
    outer = slice(size - 8, size)
    for a in range(4):
        la, lb = low_of(ya[a, outer], yb[a, outer]), low_of(ya[a + 4, outer], yb[a + 4, outer])
        ha, hb = high_of(ya[a, outer], yb[a, outer]), high_of(ya[a + 4, outer], yb[a + 4, outer])
        lo, hi = split(la, lb, 0), split(ha, hb, 1)
        for k in range(4):
            w[a * 4 + k, 0:1] = lo[k : k + 1]
            w[a * 4 + k, 13:14] = hi[k : k + 1]

    scale = smooth_weight / 4.0
    stop = (lane == 63) | (lane == 127)

    def face_turn(x):
        v = w[x]
        mlev[0, x] = face(v, roll(v, -1, 0), scale)
        mlev[1, x] = jnp.where(stop, 0.0, face(v, roll(v, -1, 1), scale))

    loop(0, 16, face_turn)

    def across_turn(x):
        mfx[x + 1] = face(w[x], w[x + 1], scale)

    loop(0, 15, across_turn)
    seam_face = jnp.where(lane < 64, face(w[15], roll(w[0], 64, 1), scale), 0.0)
    mfx[16] = seam_face
    mfx[0] = roll(seam_face, 64, 1)

    if not first:
        mtens_copy.wait()

    def inverse_turn(x):
        total = total_of(mfx[x + 1], mfx[x], mlev[0, x], mlev[1, x])
        inv = inverse_sym([mtens[k, x] for k in range(6)], total)
        for k in range(6):
            mlev[2 + k, x] = inv[k]
        begin = apply_sym(inv, [mlev[8 + c, x] for c in range(3)])
        for c in range(3):
            u1[c, x + 1] = begin[c]

    loop(0, 16, inverse_turn)
    seam(u1)
    far = [(mfx, mfx_far), (mlev, mlev_far)]
    copies = moved(far + [(mtens, mtens_far)] if first else far, sems)
    bufs = (u1, err)
    for n in range(SWEEPS - 1):
        mid_sweep(bufs[n % 2], bufs[(n + 1) % 2], mfx, mlev)
    (err_copy,) = moved([(err, err_far)], sems.at[3:4])
    count = stage.shape[0] // 4
    stage[...] = jnp.zeros(stage.shape, jnp.float32)

    def rest_turn(a):
        sums = [jnp.zeros(shape, jnp.float32) for _ in range(9 if first else 3)]
        for k in range(4):
            x = a * 4 + k
            fx_up, fx_down = mfx[x + 1], mfx[x]
            fy, fz = mlev[0, x], mlev[1, x]
            total = total_of(fx_up, fx_down, fy, fz)
            here = [err[c, x + 1] for c in range(3)]
            moved = apply_sym([mtens[k, x] for k in range(6)], here)
            for c in range(3):
                sums[c] = sums[c] + (
                    mlev[8 + c, x]
                    + inflow(here[c], err[c, x + 2], err[c, x], fx_up, fx_down, fy, fz)
                    - moved[c]
                    - total * here[c]
                )
            if first:
                for q in range(6):
                    sums[3 + q] = sums[3 + q] + mtens[q, x]
        for q, v in enumerate(sums):
            stage[a * count + q : a * count + q + 1] = jnp.sum(v[5:9], axis=0, keepdims=True)

    loop(0, 4, rest_turn)
    for c in range(3):
        for x in range(16):
            v = err[c, x + 1, 5:9]
            to_a[3 + c, x] = v
            to_b[3 + c, x] = v
    square = (128, 128)
    z, to = iota(square, 0), iota(square, 1)
    gather = jnp.where((z // 64 == to // 64) & ((z % 64) // 4 == to % 64), 1.0 / 64.0, 0.0)
    mixed = dot(stage[...], gather)
    value = mixed[0:count]
    for a in range(1, 4):
        value = value + roll(mixed[a * count : (a + 1) * count], 16 * a, 1)
    value = value[0 : msg.shape[1]]
    for s in range(32):
        msg[s] = value
    for copy in [*copies, err_copy]:
        copy.wait()


def coarse_kernel(first, *refs):
    if first:
        par, whole, mfx_far, mlev_far, err_far, ea, eb, out, cinv_far, mfx, mlev, err, cinv, u0, u1, lifted, sems = refs
    else:
        par, whole, mfx_far, mlev_far, err_far, ea, eb, cinv, out, mfx, mlev, err, u0, u1, lifted, sems = refs
    copies = moved([(mfx_far, mfx), (mlev_far, mlev), (err_far, err)], sems)
    count = whole.shape[0] // 32
    grid = (32, 128)
    row, lane = iota(grid, 0), iota(grid, 1)
    cx, cz = lane // 16, lane % 16
    scale = smooth_weight / 64.0
    one = lambda cond: jnp.where(cond, scale, 0.0)
    ups = (one(cx < 7), one(cx > 0), one(row < 31), one(row > 0), one(cz < 15), one(cz > 0))
    total = ups[0] + ups[1] + ups[2] + ups[3] + ups[4] + ups[5]
    if first:
        inv = inverse_sym([whole[pl.ds(3 + k, 32, stride=count), :] for k in range(6)], total)
        for k in range(6):
            cinv[k] = inv[k]
        copies += moved([(cinv, cinv_far)], sems.at[3:4])
    inv = [cinv[k] for k in range(6)]
    source = [whole[pl.ds(c, 32, stride=count), :] for c in range(3)]

    def turn(index, now):
        flux = []
        for c in range(3):
            v = now[c]
            flux.append(
                source[c]
                + ups[0] * roll(v, -16, 1)
                + ups[1] * roll(v, 16, 1)
                + ups[2] * roll(v, -1, 0)
                + ups[3] * roll(v, 1, 0)
                + ups[4] * roll(v, -1, 1)
                + ups[5] * roll(v, 1, 1)
            )
        step = apply_sym(inv, flux)
        return tuple((1.0 - damping) * now[c] + step[c] for c in range(3))

    correction = lax.fori_loop(0, COARSE_SWEEPS - 1, turn, tuple(apply_sym(inv, source)))

    shape = (MROWS, 32)
    place = (iota(shape, 0) + (par[1] * 4 - 5)).astype(jnp.float32) * 0.25 - 0.375
    along = hat(place - iota(shape, 1).astype(jnp.float32))
    rows = jnp.concatenate([dot(along, correction[c]) for c in range(3)], axis=0)
    square = (128, 128)
    src, to = iota(square, 0), iota(square, 1)
    depth = hat((to % 64).astype(jnp.float32) * 0.25 - 0.375 - (src % 16).astype(jnp.float32))
    for a in range(4):
        spread = jnp.where(src // 16 == a + 4 * (to // 64), depth, 0.0)
        lifted[a + 1] = dot(rows, spread)
    halves = iota((3 * MROWS, 128), 1) < 64
    lifted[0] = jnp.where(halves, 0.0, roll(lifted[4], 64, 1))
    lifted[5] = jnp.where(halves, roll(lifted[1], 64, 1), 0.0)

    for copy in copies:
        copy.wait()
    low_of, high_of = sides(par, 1, (4, 128))
    zero = jnp.zeros((MROWS, 128), jnp.float32)
    for x in range(16):
        a, d = x // 4, x % 4
        t = (d + 0.5) / 4 - 0.5
        other = a if t < 0 else a + 2
        added = (1.0 - abs(t)) * lifted[a + 1] + abs(t) * lifted[other]
        for c in range(3):
            u0[c, x + 1] = zero
            u0[c, x + 1, 1:5] = low_of(ea[3 + c, x], eb[3 + c, x])
            u0[c, x + 1, 5:9] = err[c, x + 1, 5:9]
            u0[c, x + 1, 9:13] = high_of(ea[3 + c, x], eb[3 + c, x])
            u0[c, x + 1] = u0[c, x + 1] + added[c * MROWS : (c + 1) * MROWS]
    seam(u0)
    bufs = (u0, u1)
    for n in range(SWEEPS):
        mid_sweep(bufs[n % 2], bufs[(n + 1) % 2], mfx, mlev)

    left = iota((4, 128), 1) < 64
    for b in range(3):
        block = par[0] + (b - 1)
        there = jnp.where((block >= 0) & (block < 8), 1.0, 0.0)
        block = jnp.clip(block, 0, 7)
        upper = (jnp.zeros((4, 128), jnp.int32) + block // 4) == 1
        for k in range(4):
            x = (block % 4) * 4 + k + 1
            v = [u0[c, x, 5:9] for c in range(3)]
            v = [(a, roll(a, 64, 1)) for a in v]
            to_left = [jnp.where(upper, turned, a) for a, turned in v]
            to_right = [jnp.where(upper, a, turned) for a, turned in v]
            out[0, b * 4 + k] = jnp.where(left, to_left[0], to_right[1]) * there
            out[1, b * 4 + k] = jnp.where(left, to_left[2], 0.0) * there


def post_kernel(par, flow, fa, fb, ya, yb, mine, ea, eb, lev_far, tens_far, out, lev, tens, u0, u1, mixed, lifted, tall, sems):
    copies = moved(
        [(lev_far.at[:, 2:17], lev.at[:, 2:17]), (tens_far.at[6:9, 3:17], tens.at[6:9, 3:17])], sems
    )
    low_of, high_of = sides(par, 1, (4, 128))
    zero = jnp.zeros((4, 128), jnp.float32)

    def place(c, k, v):
        u0[c, 2 + k, 8:16] = v

    wide_layers(par, flow, fa, fb, place)

    def edge_turn(k):
        for c in range(3):
            u0[c, 2 + k, 0:4] = zero
            u0[c, 2 + k, 4:8] = low_of(ya[c, k], yb[c, k])
            u0[c, 2 + k, 16:20] = high_of(ya[c, k], yb[c, k])
            u0[c, 2 + k, 20:24] = zero

    loop(0, 16, edge_turn)
    for x in range(12):
        for p in range(2):
            v = [low_of(ea[p, x], eb[p, x]), mine[p, x], high_of(ea[p, x], eb[p, x])]
            for q in range(3):
                mixed[2 * p, x, 4 * q : 4 * q + 4] = v[q]
            mixed[2 * p, x, 12:16] = zero
    square = (128, 128)
    src, to = iota(square, 0), iota(square, 1)
    place = to.astype(jnp.float32) * 0.5 - 0.25
    depth = hat(place - (src % 64).astype(jnp.float32))
    low = jnp.where(src < 64, depth, 0.0)
    high = jnp.where(src < 64, 0.0, depth)
    for c in range(3):
        v = mixed[2 * (c // 2)].reshape(12 * 16, 128)
        lifted[c] = dot(v, high if c == 1 else low).reshape(12, 16, 128)

    def tall_turn(x):
        for c in range(3):
            v = lifted[c, x]
            tall[c, x, pl.ds(0, 12, stride=2), :] = (0.75 * v + 0.25 * roll(v, 1, 0))[0:12]
            tall[c, x, pl.ds(1, 12, stride=2), :] = (0.75 * v + 0.25 * roll(v, -1, 0))[0:12]

    loop(0, 12, tall_turn)

    def add_turn(m):
        for c in range(3):
            a, b, d = tall[c, m - 1], tall[c, m], tall[c, m + 1]
            x = 2 * m - 2
            u0[c, x] = u0[c, x] + (0.75 * b + 0.25 * a)
            u0[c, x + 1] = u0[c, x + 1] + (0.75 * b + 0.25 * d)

    loop(2, 10, add_turn)
    for copy in copies:
        copy.wait()
    bufs = (u0, u1)
    for n in range(SWEEPS):
        fine_sweep(bufs[n % 2], bufs[(n + 1) % 2], 3 + n, 17 - n, lev, tens)
    for c in range(3):
        for k in range(8):
            out[c, k] = u0[c, 6 + k, 8:16]


def f32(*shape):
    return jax.ShapeDtypeStruct(shape, jnp.float32)


def call(kernel, outs, scratch, args, far_in=(), far_out=(), sems=0):
    near, far = pl.BlockSpec(memory_space=pltpu.VMEM), pl.BlockSpec(memory_space=pltpu.HBM)
    args = [pltpu.with_memory_space_constraint(v, pltpu.HBM) if k in far_in else v for k, v in enumerate(args)]
    specs = [pl.BlockSpec(memory_space=pltpu.SMEM)]
    specs += [far if k in far_in else near for k in range(1, len(args))]
    scratch_shapes = [pltpu.VMEM(shape, jnp.float32) for shape in scratch]
    if sems:
        scratch_shapes.append(pltpu.SemaphoreType.DMA((sems,)))
    return pl.pallas_call(
        kernel,
        in_specs=specs,
        out_specs=[far if k in far_out else near for k in range(len(outs))],
        out_shape=[pltpu.HBM(shape, jnp.float32) if k in far_out else f32(*shape) for k, shape in enumerate(outs)],
        scratch_shapes=scratch_shapes,
        compiler_params=pltpu.CompilerParams(vmem_limit_bytes=24 * 2**20),
        cost_estimate=pl.CostEstimate(flops=20_000_000, bytes_accessed=1_000_000, transcendentals=0),
    )(*args)


def pairs_of(size, start):
    pairs = []
    for k in range(start, size - 1, 2):
        pairs += [(k, k + 1), (k + 1, k)]
    return pairs


def across(field, axes, start):
    return lax.ppermute(field, axes, pairs_of(lax.axis_size(axes), start))


def beside(field, axes):
    return [across(field, axes, 0), across(field, axes, 1)]


def shared(message, axes):
    return lax.all_to_all(message, axes, 0, 0, tiled=True)


def body(first_image, second_image, start_flow):
    par = jnp.stack([lax.axis_index(GX), lax.axis_index(GY)]).astype(jnp.int32)
    block = jnp.concatenate([start_flow, first_image[None], second_image[None]])
    flow = start_flow
    tens = mtens = cinv = None
    fine_shape, mid_shape = (WIDE, ROWS, 128), (16, MROWS, 128)
    for cycle in range(CYCLES):
        first = cycle == 0
        sent = block if first else flow
        fields = sent.shape[0]
        args = [par, sent, *beside(sent, GX)]
        outs = [(fields, WIDE, 8, 128), (fields, 28, 4, 128), (fields, 28, 4, 128)]
        wide, to_a, to_b = call(widen_kernel, outs, [], args)
        size = 88 if first else 40
        stage = (6 if first else 3) * 32
        outs = [(3, 8, 8, 128), (8, size, 128), (9, *fine_shape)]
        scratch = [(9, *fine_shape), (9, *fine_shape), (fields, *fine_shape), (3, *fine_shape), fine_shape]
        scratch += [(stage, 128)] * 3
        args = [par, wide, across(to_a, GY, 0), across(to_b, GY, 1)]
        pre = functools.partial(pre_kernel, first)
        if first:
            flow, message, lev, tens = call(pre, [*outs, (9, *fine_shape)], scratch, args, (), (2, 3), 2)
        else:
            flow, message, lev = call(pre, outs, scratch, [*args, tens], (4,), (2,), 2)
        layers = beside(flow, GX)
        mids = shared(message, GX)
        args = [par, mids, *beside(mids, GY), flow, *layers]
        count, padded = (12, 16) if first else (4, 8)
        sides_shape = (6, 16, 4, 128)
        saved = [(17, MROWS, 128), (11, *mid_shape), (3, 18, MROWS, 128)]
        outs = [(32, count, 128), sides_shape, sides_shape, *saved]
        scratch = [*saved, (6, *mid_shape), (3, 18, MROWS, 128), mid_shape, (4 * padded, 128)]
        mid = functools.partial(mid_kernel, first)
        if first:
            coarse, to_a, to_b, mfx, mlev, err, mtens = call(
                mid, [*outs, (6, *mid_shape)], scratch, args, (), (3, 4, 5, 6), 4
            )
        else:
            coarse, to_a, to_b, mfx, mlev, err = call(mid, outs, scratch, [*args, mtens], (7,), (3, 4, 5), 4)
        edges = [across(to_a, GY, 0), across(to_b, GY, 1)]
        whole = shared(coarse, GY).reshape(32 * count, 128)
        args = [par, whole, mfx, mlev, err, *edges]
        outs = [(2, 12, 4, 128)]
        scratch = [(3, 18, MROWS, 128), (3, 18, MROWS, 128), (6, 3 * MROWS, 128)]
        inverse = (6, 32, 128)
        low = functools.partial(coarse_kernel, first)
        if first:
            error, cinv = call(low, [*outs, inverse], [*saved, inverse, *scratch], args, (2, 3, 4), (1,), 4)
        else:
            (error,) = call(low, outs, [*saved, *scratch], [*args, cinv], (2, 3, 4), (), 4)
        args = [par, flow, *layers, *edges, error, *beside(error, GY), lev, tens]
        scratch = [(9, *fine_shape), (9, *fine_shape), (3, *fine_shape), (3, *fine_shape)]
        scratch += [(3, 12, 16, 128), (3, 12, 16, 128), (3, 12, 24, 128)]
        (flow,) = call(post_kernel, [(3, 8, 8, 128)], scratch, args, (9, 10), (), 2)
    return flow


def solution(mesh):
    finer = Mesh(mesh.devices.reshape(4, 2, 8, 4), ("gx_0", "gx_1", "gy_0", "gy_1"))
    return jax.shard_map(
        body,
        mesh=finer,
        in_specs=(P(GX, GY, None), P(GX, GY, None), P(None, GX, GY, None)),
        out_specs=P(None, GX, GY, None),
        check_vma=False,
    )
```

```python
import functools

import jax
import jax.numpy as jnp
from jax import lax
from jax.experimental import pallas as pl
from jax.experimental.pallas import tpu as pltpu
from jax.sharding import Mesh
from jax.sharding import PartitionSpec as P


SWEEPS = 4
COARSE_SWEEPS = 12
CYCLES = 2
GX = ("gx_0", "gx_1")
GY = ("gy_0", "gy_1")

damping = 0.6
smooth_weight = 2.0
floor_grad = 0.5

NX, NY = 64, 256
ROWS = 24
NEAR = slice(4, 20)
WIDE = 20
MROWS = 16


def roll(v, shift, axis):
    return pltpu.roll(v, shift % v.shape[axis], axis)


def iota(shape, dim):
    return lax.broadcasted_iota(jnp.int32, shape, dim)


def face(a, b, scale):
    summed = a + b
    return (2.0 * scale) * a * b / jnp.where(summed > 0.0, summed, 1.0)


def inverse_sym(tensor, total):
    aaa = tensor[0] + total
    bbb = tensor[1]
    ccc = tensor[2]
    ddd = tensor[3] + total
    eee = tensor[4]
    fff = tensor[5] + total
    cof_a = ddd * fff - eee * eee
    cof_b = ccc * eee - bbb * fff
    cof_c = bbb * eee - ccc * ddd
    cof_d = aaa * fff - ccc * ccc
    cof_e = bbb * ccc - aaa * eee
    cof_f = aaa * ddd - bbb * bbb
    determinant = aaa * cof_a + bbb * cof_b + ccc * cof_c
    share = jnp.where(total > 0.0, damping / determinant, 0.0)
    return [cof * share for cof in (cof_a, cof_b, cof_c, cof_d, cof_e, cof_f)]


def apply_sym(m, v):
    return [
        m[0] * v[0] + m[1] * v[1] + m[2] * v[2],
        m[1] * v[0] + m[3] * v[1] + m[4] * v[2],
        m[2] * v[0] + m[4] * v[1] + m[5] * v[2],
    ]


def inflow(here, above, below, fx_up, fx_down, fy, fz):
    return (
        fx_up * above
        + fx_down * below
        + fy * roll(here, -1, 0)
        + roll(fy * here, 1, 0)
        + fz * roll(here, -1, 1)
        + roll(fz * here, 1, 1)
    )


def total_of(fx_up, fx_down, fy, fz):
    return fx_up + fx_down + fy + roll(fy, 1, 0) + fz + roll(fz, 1, 1)


def loop(low, high, turn):
    for index in range(low, high):
        turn(index)


def moved(pairs, sems):
    copies = [pltpu.make_async_copy(a, b, sems.at[k]) for k, (a, b) in enumerate(pairs)]
    for copy in copies:
        copy.start()
    return copies


def sides(par, which, shape):
    is_odd = (jnp.zeros(shape, jnp.int32) + (par[which] & 1)) == 1
    return (lambda a, b: jnp.where(is_odd, a, b)), (lambda a, b: jnp.where(is_odd, b, a))


def hat(distance):
    return jnp.maximum(1.0 - jnp.abs(distance), 0.0)


def dot(a, b):
    return jnp.dot(a, b, precision=lax.Precision.HIGHEST, preferred_element_type=jnp.float32)


def fine_sweep(source, target, low, high, lev, tens):
    def turn(x):
        fx_up, fx_down = lev[0, x], lev[0, x - 1]
        fy, fz = lev[1, x], lev[2, x]
        here = [source[c, x] for c in range(3)]
        flux = [
            tens[6 + c, x]
            + inflow(here[c], source[c, x + 1], source[c, x - 1], fx_up, fx_down, fy, fz)
            for c in range(3)
        ]
        step = apply_sym([lev[3 + k, x] for k in range(6)], flux)
        for c in range(3):
            target[c, x] = (1.0 - damping) * here[c] + step[c]

    loop(low, high, turn)


def widen_kernel(par, own, xa, xb, wide, to_a, to_b):
    low_of, high_of = sides(par, 0, (8, 128))
    first_of, second_of = sides(par, 1, (4, 128))
    for f in range(own.shape[0]):
        for x in range(WIDE):
            if x < 6:
                v = low_of(xa[f, 2 + x], xb[f, 2 + x])
            elif x < 14:
                v = own[f, x - 6]
            else:
                v = high_of(xa[f, x - 14], xb[f, x - 14])
            wide[f, x] = v
            below, above = v[0:4], v[4:8]
            if 1 <= x < 19:
                to_a[f, x - 1] = first_of(below, above)
                to_b[f, x - 1] = second_of(below, above)
            if 5 <= x < 15:
                to_a[f, 13 + x] = first_of(above, below)
                to_b[f, 13 + x] = second_of(above, below)


def stack_rows(par, own, ya, yb, out, close):
    low_of, high_of = sides(par, 1, (4, 128))
    zero = jnp.zeros((4, 128), jnp.float32)
    for f in range(own.shape[0]):
        for x in range(WIDE):
            out[f, x, 8:16] = own[f, x]
            near = (ya[f, x - 1], yb[f, x - 1]) if 1 <= x < 19 else (zero, zero)
            far = (ya[f, 13 + x], yb[f, 13 + x]) if 5 <= x < 15 else (zero, zero)
            low, high = low_of(*near), high_of(*near)
            out[f, x, 0:4] = low_of(*far)
            out[f, x, 4:8] = low
            out[f, x, 16:20] = high
            out[f, x, 20:24] = high_of(*far)
            if f < 3:
                close[f, x, 0:4] = low
                close[f, x, 4:12] = own[f, x]
                close[f, x, 12:16] = high


def pre_kernel(first, *refs):
    if first:
        par, own, ya, yb, flow_out, msg, lev_far, tens_far, lev, tens, full, u0, u1, w, fy_low, even, odd, sums, sems = refs
    else:
        par, own, ya, yb, tens, flow_out, msg, lev_far, lev, full, u0, u1, w, fy_low, even, odd, sums, sems = refs
    shape = (ROWS, 128)
    lane = iota(shape, 1)
    last, start = lane == 127, lane == 0
    stack_rows(par, own, ya, yb, full, u0)
    near_last = iota((16, 128), 1) == 127

    def z_slope(v):
        return jnp.where(last, 0.0, roll(v, -1, 1)) - jnp.where(start, 0.0, roll(v, 1, 1))

    def y_slope(v):
        return roll(v, -1, 0) - roll(v, 1, 0)

    if first:

        def tensor_turn(x):
            mean = 0.5 * (full[3, x] + full[4, x])
            sx = 0.25 * ((full[3, x + 1] + full[4, x + 1]) - (full[3, x - 1] + full[4, x - 1]))
            sy = 0.5 * y_slope(mean)
            sz = 0.5 * z_slope(mean)
            change = full[4, x] - full[3, x]
            scale = 1.0 / (sx * sx + sy * sy + sz * sz + floor_grad)
            gx, gy, gz = scale * sx, scale * sy, scale * sz
            for k, v in enumerate((gx * sx, gx * sy, gx * sz, gy * sy, gy * sz, gz * sz)):
                tens[k, x] = v[NEAR]
            for k, v in enumerate((gx, gy, gz)):
                tens[6 + k, x] = (-v * change)[NEAR]

        loop(2, 18, tensor_turn)

    row = iota(shape, 0) + (par[1] * 8 - 8)
    inside_y = (row >= 0) & (row < NY)

    def weight_turn(x):
        total = jnp.ones(shape, jnp.float32)
        for c in range(3):
            v = full[c, x]
            for slope in (full[c, x + 1] - full[c, x - 1], y_slope(v), z_slope(v)):
                total = total + slope * slope
        place = x + (par[0] * 8 - 6)
        keep = jnp.where((place >= 0) & (place < NX), 1.0, 0.0)
        w[x] = jnp.where(inside_y, lax.rsqrt(total), 0.0) * keep

    loop(1, 19, weight_turn)

    def face_turn(x):
        v = w[x]
        near = v[NEAR]
        lev[0, x] = face(near, w[x + 1][NEAR], smooth_weight)
        if x > 1:
            along = face(v, roll(v, -1, 0), smooth_weight)
            lev[1, x] = along[NEAR]
            fy_low[x] = along[3:19]
            lev[2, x] = jnp.where(near_last, 0.0, face(near, roll(near, -1, 1), smooth_weight))

    loop(1, 18, face_turn)

    def inverse_turn(x):
        fz = lev[2, x]
        total = lev[0, x] + lev[0, x - 1] + lev[1, x] + fy_low[x] + fz + roll(fz, 1, 1)
        for k, v in enumerate(inverse_sym([tens[k, x] for k in range(6)], total)):
            lev[3 + k, x] = v

    loop(2, 18, inverse_turn)
    far = [(lev, lev_far), (tens, tens_far)] if first else [(lev, lev_far)]
    copies = moved(far, sems)
    bufs = (u0, u1)


    def first_turn(x):
        fx_up, fx_down = lev[0, x], lev[0, x - 1]
        fy, fz = lev[1, x], lev[2, x]
        here = [u0[c, x] for c in range(3)]
        flux = [
            tens[6 + c, x]
            + fx_up * u0[c, x + 1]
            + fx_down * u0[c, x - 1]
            + fy * full[c, x, 5:21]
            + fy_low[x] * full[c, x, 3:19]
            + fz * roll(here[c], -1, 1)
            + roll(fz * here[c], 1, 1)
            for c in range(3)
        ]
        step = apply_sym([lev[3 + k, x] for k in range(6)], flux)
        for c in range(3):
            u1[c, x] = (1.0 - damping) * here[c] + step[c]

    loop(2, 18, first_turn)
    for n in range(1, SWEEPS):
        fine_sweep(bufs[n % 2], bufs[(n + 1) % 2], 2 + n, 18 - n, lev, tens)

    def rest_at(x):
        fx_up, fx_down = lev[0, x], lev[0, x - 1]
        fy, fz = lev[1, x], lev[2, x]
        total = total_of(fx_up, fx_down, fy, fz)
        here = [u0[c, x] for c in range(3)]
        moved = apply_sym([tens[k, x] for k in range(6)], here)
        return [
            (
                tens[6 + c, x]
                + inflow(here[c], u0[c, x + 1], u0[c, x - 1], fx_up, fx_down, fy, fz)
                - moved[c]
                - total * here[c]
            )[4:12]
            for c in range(3)
        ]

    def rest_turn(m):
        x = 6 + 2 * m
        rest = [a + b for a, b in zip(rest_at(x), rest_at(x + 1))]
        pair = w[x] + w[x + 1]
        fields = rest + [pair[8:16], roll(pair, 2, 0)[8:16], pair[16:24]]
        if first:
            fields += [tens[k, x, 4:12] + tens[k, x + 1, 4:12] for k in range(6)]
        for k, v in enumerate(fields):
            stage = odd if k % 2 else even
            at = (k // 2) * 32 + m * 8
            stage[at : at + 8] = v

    loop(0, 4, rest_turn)
    for c in range(3):
        for k in range(8):
            flow_out[c, k] = u0[c, 6 + k, 4:12]
    square = (128, 128)
    into = iota(square, 0) // 2
    low = jnp.where(into == iota(square, 1), 0.125, 0.0)
    high = jnp.where(into + 64 == iota(square, 1), 0.125, 0.0)
    sums[...] = dot(even[...], low) + dot(odd[...], high)
    pairs = even.shape[0] // 32
    size = msg.shape[1]
    at = 0
    for p in range(pairs):
        if p == 2:
            v = sums[pl.ds(64, 4, stride=8), :] + sums[pl.ds(65, 4, stride=8), :]
            for s in range(8):
                msg[s, size - 8 : size - 4] = v
                msg[s, size - 4 : size] = v
            continue
        v = sums[pl.ds(p * 32, 16, stride=2), :] + sums[pl.ds(p * 32 + 1, 16, stride=2), :]
        for s in range(8):
            msg[s, at : at + 16] = v
        at += 16
    for copy in copies:
        copy.wait()


def wide_layers(par, own, xa, xb, place):
    low_of, high_of = sides(par, 0, (8, 128))
    for c in range(3):
        for k in range(4):
            place(c, k, low_of(xa[c, 4 + k], xb[c, 4 + k]))
            place(c, 12 + k, high_of(xa[c, k], xb[c, k]))
        for k in range(8):
            place(c, 4 + k, own[c, k])


def send_flow(par, flow, fa, fb, to_a, to_b):
    first_of, second_of = sides(par, 1, (4, 128))

    def place(c, k, v):
        to_a[c, k] = first_of(v[0:4], v[4:8])
        to_b[c, k] = second_of(v[0:4], v[4:8])

    wide_layers(par, flow, fa, fb, place)


def mid_sweep(source, target, mfx, mlev):
    def turn(x):
        fx_up, fx_down = mfx[x + 1], mfx[x]
        fy, fz = mlev[0, x], mlev[1, x]
        here = [source[c, x + 1] for c in range(3)]
        flux = [
            mlev[8 + c, x]
            + inflow(here[c], source[c, x + 2], source[c, x], fx_up, fx_down, fy, fz)
            for c in range(3)
        ]
        step = apply_sym([mlev[2 + k, x] for k in range(6)], flux)
        for c in range(3):
            target[c, x + 1] = (1.0 - damping) * here[c] + step[c]

    loop(0, 16, turn)
    seam(target)


def seam(field):
    for c in range(3):
        field[c, 0] = roll(field[c, 16], 64, 1)
        field[c, 17] = roll(field[c, 1], 64, 1)


def mid_kernel(first, *refs):
    if first:
        par, own, ya, yb, flow, fa, fb, msg, to_a, to_b, *refs = refs
        mfx_far, mlev_far, err_far, mtens_far, mfx, mlev, err, mtens, u1, w, stage, sems = refs
    else:
        par, own, ya, yb, flow, fa, fb, mtens, msg, to_a, to_b, *refs = refs
        mfx_far, mlev_far, err_far, mfx, mlev, err, u1, w, stage, sems = refs
    send_flow(par, flow, fa, fb, to_a, to_b)
    shape = (MROWS, 128)
    lane = iota(shape, 1)
    left = iota((8, 128), 1) < 64
    low_of, high_of = sides(par, 1, (8, 128))
    size = own.shape[1]
    zero4 = jnp.zeros((4, 128), jnp.float32)

    def split(a, b, which):
        if which:
            return jnp.where(left, roll(a, 64, 1), b)
        return jnp.where(left, a, roll(b, 64, 1))

    def fields_of(out, slot, pair, which):
        def turn(a):
            for kk in range(2):
                rows = slice(pair * 16 + kk * 8, pair * 16 + kk * 8 + 8)
                la, lb = low_of(ya[a, rows], yb[a, rows]), low_of(ya[a + 4, rows], yb[a + 4, rows])
                ha, hb = high_of(ya[a, rows], yb[a, rows]), high_of(ya[a + 4, rows], yb[a + 4, rows])
                for base, va, vb in ((1, la, lb), (5, own[a, rows], own[a + 4, rows]), (9, ha, hb)):
                    v = split(va, vb, which)
                    for k in range(2):
                        x = a * 4 + kk * 2 + k
                        if slot is None:
                            out[x, base : base + 4] = v[4 * k : 4 * k + 4]
                        else:
                            out[slot, x, base : base + 4] = v[4 * k : 4 * k + 4]

        loop(0, 4, turn)

    def clear_turn(x):
        for ref in (w,):
            ref[x, 0:1] = zero4[0:1]
            ref[x, 13:16] = zero4[0:3]
        for k in range(3):
            mlev[8 + k, x, 0:1] = zero4[0:1]
            mlev[8 + k, x, 13:16] = zero4[0:3]
        if first:
            for k in range(6):
                mtens[k, x, 0:1] = zero4[0:1]
                mtens[k, x, 13:16] = zero4[0:3]

    loop(0, 16, clear_turn)
    fields_of(mlev, 8, 0, 0)
    fields_of(mlev, 9, 0, 1)
    fields_of(mlev, 10, 1, 0)
    fields_of(w, None, 1, 1)
    if first:
        for k in range(6):
            fields_of(mtens, k, 2 + k // 2, k % 2)
    outer = slice(size - 8, size)
    for a in range(4):
        la, lb = low_of(ya[a, outer], yb[a, outer]), low_of(ya[a + 4, outer], yb[a + 4, outer])
        ha, hb = high_of(ya[a, outer], yb[a, outer]), high_of(ya[a + 4, outer], yb[a + 4, outer])
        lo, hi = split(la, lb, 0), split(ha, hb, 1)
        for k in range(4):
            w[a * 4 + k, 0:1] = lo[k : k + 1]
            w[a * 4 + k, 13:14] = hi[k : k + 1]

    scale = smooth_weight / 4.0
    stop = (lane == 63) | (lane == 127)

    def face_turn(x):
        v = w[x]
        mlev[0, x] = face(v, roll(v, -1, 0), scale)
        mlev[1, x] = jnp.where(stop, 0.0, face(v, roll(v, -1, 1), scale))

    loop(0, 16, face_turn)

    def across_turn(x):
        mfx[x + 1] = face(w[x], w[x + 1], scale)

    loop(0, 15, across_turn)
    seam_face = jnp.where(lane < 64, face(w[15], roll(w[0], 64, 1), scale), 0.0)
    mfx[16] = seam_face
    mfx[0] = roll(seam_face, 64, 1)

    def inverse_turn(x):
        total = total_of(mfx[x + 1], mfx[x], mlev[0, x], mlev[1, x])
        inv = inverse_sym([mtens[k, x] for k in range(6)], total)
        for k in range(6):
            mlev[2 + k, x] = inv[k]
        begin = apply_sym(inv, [mlev[8 + c, x] for c in range(3)])
        for c in range(3):
            u1[c, x + 1] = begin[c]

    loop(0, 16, inverse_turn)
    seam(u1)
    far = [(mfx, mfx_far), (mlev, mlev_far)]
    copies = moved(far + [(mtens, mtens_far)] if first else far, sems)
    bufs = (u1, err)
    for n in range(SWEEPS - 1):
        mid_sweep(bufs[n % 2], bufs[(n + 1) % 2], mfx, mlev)
    (err_copy,) = moved([(err, err_far)], sems.at[3:4])
    count = stage.shape[0] // 4
    stage[...] = jnp.zeros(stage.shape, jnp.float32)

    def rest_turn(a):
        sums = [jnp.zeros(shape, jnp.float32) for _ in range(9 if first else 3)]
        for k in range(4):
            x = a * 4 + k
            fx_up, fx_down = mfx[x + 1], mfx[x]
            fy, fz = mlev[0, x], mlev[1, x]
            total = total_of(fx_up, fx_down, fy, fz)
            here = [err[c, x + 1] for c in range(3)]
            moved = apply_sym([mtens[k, x] for k in range(6)], here)
            for c in range(3):
                sums[c] = sums[c] + (
                    mlev[8 + c, x]
                    + inflow(here[c], err[c, x + 2], err[c, x], fx_up, fx_down, fy, fz)
                    - moved[c]
                    - total * here[c]
                )
            if first:
                for q in range(6):
                    sums[3 + q] = sums[3 + q] + mtens[q, x]
        for q, v in enumerate(sums):
            stage[a * count + q : a * count + q + 1] = jnp.sum(v[5:9], axis=0, keepdims=True)

    loop(0, 4, rest_turn)
    for c in range(3):
        for x in range(16):
            v = err[c, x + 1, 5:9]
            to_a[3 + c, x] = v
            to_b[3 + c, x] = v
    square = (128, 128)
    z, to = iota(square, 0), iota(square, 1)
    gather = jnp.where((z // 64 == to // 64) & ((z % 64) // 4 == to % 64), 1.0 / 64.0, 0.0)
    mixed = dot(stage[...], gather)
    value = mixed[0:count]
    for a in range(1, 4):
        value = value + roll(mixed[a * count : (a + 1) * count], 16 * a, 1)
    value = value[0 : msg.shape[1]]
    for s in range(32):
        msg[s] = value
    for copy in [*copies, err_copy]:
        copy.wait()


def coarse_kernel(first, *refs):
    if first:
        par, whole, mfx_far, mlev_far, err_far, ea, eb, out, cinv_far, mfx, mlev, err, cinv, u0, u1, lifted, sems = refs
    else:
        par, whole, mfx_far, mlev_far, err_far, ea, eb, cinv, out, mfx, mlev, err, u0, u1, lifted, sems = refs
    copies = moved([(mfx_far, mfx), (mlev_far, mlev), (err_far, err)], sems)
    count = whole.shape[0] // 32
    grid = (32, 128)
    row, lane = iota(grid, 0), iota(grid, 1)
    cx, cz = lane // 16, lane % 16
    scale = smooth_weight / 64.0
    one = lambda cond: jnp.where(cond, scale, 0.0)
    ups = (one(cx < 7), one(cx > 0), one(row < 31), one(row > 0), one(cz < 15), one(cz > 0))
    total = ups[0] + ups[1] + ups[2] + ups[3] + ups[4] + ups[5]
    if first:
        inv = inverse_sym([whole[pl.ds(3 + k, 32, stride=count), :] for k in range(6)], total)
        for k in range(6):
            cinv[k] = inv[k]
        copies += moved([(cinv, cinv_far)], sems.at[3:4])
    inv = [cinv[k] for k in range(6)]
    source = [whole[pl.ds(c, 32, stride=count), :] for c in range(3)]

    def turn(index, now):
        flux = []
        for c in range(3):
            v = now[c]
            flux.append(
                source[c]
                + ups[0] * roll(v, -16, 1)
                + ups[1] * roll(v, 16, 1)
                + ups[2] * roll(v, -1, 0)
                + ups[3] * roll(v, 1, 0)
                + ups[4] * roll(v, -1, 1)
                + ups[5] * roll(v, 1, 1)
            )
        step = apply_sym(inv, flux)
        return tuple((1.0 - damping) * now[c] + step[c] for c in range(3))

    correction = lax.fori_loop(0, COARSE_SWEEPS - 1, turn, tuple(apply_sym(inv, source)))

    shape = (MROWS, 32)
    place = (iota(shape, 0) + (par[1] * 4 - 5)).astype(jnp.float32) * 0.25 - 0.375
    along = hat(place - iota(shape, 1).astype(jnp.float32))
    rows = jnp.concatenate([dot(along, correction[c]) for c in range(3)], axis=0)
    square = (128, 128)
    src, to = iota(square, 0), iota(square, 1)
    depth = hat((to % 64).astype(jnp.float32) * 0.25 - 0.375 - (src % 16).astype(jnp.float32))
    for a in range(4):
        spread = jnp.where(src // 16 == a + 4 * (to // 64), depth, 0.0)
        lifted[a + 1] = dot(rows, spread)
    halves = iota((3 * MROWS, 128), 1) < 64
    lifted[0] = jnp.where(halves, 0.0, roll(lifted[4], 64, 1))
    lifted[5] = jnp.where(halves, roll(lifted[1], 64, 1), 0.0)

    for copy in copies:
        copy.wait()
    low_of, high_of = sides(par, 1, (4, 128))
    zero = jnp.zeros((MROWS, 128), jnp.float32)
    for x in range(16):
        a, d = x // 4, x % 4
        t = (d + 0.5) / 4 - 0.5
        other = a if t < 0 else a + 2
        added = (1.0 - abs(t)) * lifted[a + 1] + abs(t) * lifted[other]
        for c in range(3):
            u0[c, x + 1] = zero
            u0[c, x + 1, 1:5] = low_of(ea[3 + c, x], eb[3 + c, x])
            u0[c, x + 1, 5:9] = err[c, x + 1, 5:9]
            u0[c, x + 1, 9:13] = high_of(ea[3 + c, x], eb[3 + c, x])
            u0[c, x + 1] = u0[c, x + 1] + added[c * MROWS : (c + 1) * MROWS]
    seam(u0)
    bufs = (u0, u1)
    for n in range(SWEEPS):
        mid_sweep(bufs[n % 2], bufs[(n + 1) % 2], mfx, mlev)

    left = iota((4, 128), 1) < 64
    for b in range(3):
        block = par[0] + (b - 1)
        there = jnp.where((block >= 0) & (block < 8), 1.0, 0.0)
        block = jnp.clip(block, 0, 7)
        upper = (jnp.zeros((4, 128), jnp.int32) + block // 4) == 1
        for k in range(4):
            x = (block % 4) * 4 + k + 1
            v = [u0[c, x, 5:9] for c in range(3)]
            v = [(a, roll(a, 64, 1)) for a in v]
            to_left = [jnp.where(upper, turned, a) for a, turned in v]
            to_right = [jnp.where(upper, a, turned) for a, turned in v]
            out[0, b * 4 + k] = jnp.where(left, to_left[0], to_right[1]) * there
            out[1, b * 4 + k] = jnp.where(left, to_left[2], 0.0) * there


def post_kernel(par, flow, fa, fb, ya, yb, mine, ea, eb, lev_far, tens_far, out, lev, tens, u0, u1, mixed, lifted, tall, sems):
    copies = moved(
        [(lev_far.at[:, 2:17], lev.at[:, 2:17]), (tens_far.at[6:9, 3:17], tens.at[6:9, 3:17])], sems
    )
    low_of, high_of = sides(par, 1, (4, 128))
    zero = jnp.zeros((4, 128), jnp.float32)

    def place(c, k, v):
        u0[c, 2 + k, 4:12] = v

    wide_layers(par, flow, fa, fb, place)

    def edge_turn(k):
        for c in range(3):
            u0[c, 2 + k, 0:4] = low_of(ya[c, k], yb[c, k])
            u0[c, 2 + k, 12:16] = high_of(ya[c, k], yb[c, k])

    loop(0, 16, edge_turn)
    for x in range(12):
        for p in range(2):
            v = [low_of(ea[p, x], eb[p, x]), mine[p, x], high_of(ea[p, x], eb[p, x])]
            for q in range(3):
                mixed[2 * p, x, 4 * q : 4 * q + 4] = v[q]
            mixed[2 * p, x, 12:16] = zero
    square = (128, 128)
    src, to = iota(square, 0), iota(square, 1)
    place = to.astype(jnp.float32) * 0.5 - 0.25
    depth = hat(place - (src % 64).astype(jnp.float32))
    low = jnp.where(src < 64, depth, 0.0)
    high = jnp.where(src < 64, 0.0, depth)
    for c in range(3):
        v = mixed[2 * (c // 2)].reshape(12 * 16, 128)
        lifted[c] = dot(v, high if c == 1 else low).reshape(12, 16, 128)

    def tall_turn(x):
        for c in range(3):
            v = lifted[c, x]
            tall[c, x, pl.ds(0, 8, stride=2), :] = (0.75 * v + 0.25 * roll(v, 1, 0))[2:10]
            tall[c, x, pl.ds(1, 8, stride=2), :] = (0.75 * v + 0.25 * roll(v, -1, 0))[2:10]

    loop(1, 11, tall_turn)

    def add_turn(m):
        for c in range(3):
            a, b, d = tall[c, m - 1], tall[c, m], tall[c, m + 1]
            x = 2 * m - 2
            u0[c, x] = u0[c, x] + (0.75 * b + 0.25 * a)
            u0[c, x + 1] = u0[c, x + 1] + (0.75 * b + 0.25 * d)

    loop(2, 10, add_turn)
    for copy in copies:
        copy.wait()
    bufs = (u0, u1)
    for n in range(SWEEPS):
        fine_sweep(bufs[n % 2], bufs[(n + 1) % 2], 3 + n, 17 - n, lev, tens)
    for c in range(3):
        for k in range(8):
            out[c, k] = u0[c, 6 + k, 4:12]


def f32(*shape):
    return jax.ShapeDtypeStruct(shape, jnp.float32)


def call(kernel, outs, scratch, args, far_in=(), far_out=(), sems=0):
    near, far = pl.BlockSpec(memory_space=pltpu.VMEM), pl.BlockSpec(memory_space=pltpu.HBM)
    args = [pltpu.with_memory_space_constraint(v, pltpu.HBM) if k in far_in else v for k, v in enumerate(args)]
    specs = [pl.BlockSpec(memory_space=pltpu.SMEM)]
    specs += [far if k in far_in else near for k in range(1, len(args))]
    scratch_shapes = [pltpu.VMEM(shape, jnp.float32) for shape in scratch]
    if sems:
        scratch_shapes.append(pltpu.SemaphoreType.DMA((sems,)))
    return pl.pallas_call(
        kernel,
        in_specs=specs,
        out_specs=[far if k in far_out else near for k in range(len(outs))],
        out_shape=[pltpu.HBM(shape, jnp.float32) if k in far_out else f32(*shape) for k, shape in enumerate(outs)],
        scratch_shapes=scratch_shapes,
        compiler_params=pltpu.CompilerParams(vmem_limit_bytes=24 * 2**20),
        cost_estimate=pl.CostEstimate(flops=20_000_000, bytes_accessed=1_000_000, transcendentals=0),
    )(*args)


def pairs_of(size, start):
    pairs = []
    for k in range(start, size - 1, 2):
        pairs += [(k, k + 1), (k + 1, k)]
    return pairs


def across(field, axes, start):
    return lax.ppermute(field, axes, pairs_of(lax.axis_size(axes), start))


def beside(field, axes):
    return [across(field, axes, 0), across(field, axes, 1)]


def shared(message, axes):
    return lax.all_to_all(message, axes, 0, 0, tiled=True)


def body(first_image, second_image, start_flow):
    par = jnp.stack([lax.axis_index(GX), lax.axis_index(GY)]).astype(jnp.int32)
    block = jnp.concatenate([start_flow, first_image[None], second_image[None]])
    flow = start_flow
    tens = mtens = cinv = None
    tall_shape, fine_shape, mid_shape = (WIDE, ROWS, 128), (WIDE, 16, 128), (16, MROWS, 128)
    for cycle in range(CYCLES):
        first = cycle == 0
        sent = block if first else flow
        fields = sent.shape[0]
        args = [par, sent, *beside(sent, GX)]
        outs = [(fields, WIDE, 8, 128), (fields, 28, 4, 128), (fields, 28, 4, 128)]
        wide, to_a, to_b = call(widen_kernel, outs, [], args)
        size = 88 if first else 40
        stage = (6 if first else 3) * 32
        outs = [(3, 8, 8, 128), (8, size, 128), (9, *fine_shape)]
        scratch = [(9, *fine_shape)] * (2 if first else 1)
        scratch += [(fields, *tall_shape), (3, *fine_shape), (3, *fine_shape), tall_shape, fine_shape]
        scratch += [(stage, 128)] * 3
        args = [par, wide, across(to_a, GY, 0), across(to_b, GY, 1)]
        pre = functools.partial(pre_kernel, first)
        if first:
            flow, message, lev, tens = call(pre, [*outs, (9, *fine_shape)], scratch, args, (), (2, 3), 2)
        else:
            flow, message, lev = call(pre, outs, scratch, [*args, tens], (), (2,), 2)
        layers = beside(flow, GX)
        mids = shared(message, GX)
        args = [par, mids, *beside(mids, GY), flow, *layers]
        count, padded = (12, 16) if first else (4, 8)
        sides_shape = (6, 16, 4, 128)
        saved = [(17, MROWS, 128), (11, *mid_shape), (3, 18, MROWS, 128)]
        outs = [(32, count, 128), sides_shape, sides_shape, *saved]
        scratch = [*saved, *([(6, *mid_shape)] if first else []), (3, 18, MROWS, 128), mid_shape, (4 * padded, 128)]
        mid = functools.partial(mid_kernel, first)
        if first:
            coarse, to_a, to_b, mfx, mlev, err, mtens = call(
                mid, [*outs, (6, *mid_shape)], scratch, args, (), (3, 4, 5, 6), 4
            )
        else:
            coarse, to_a, to_b, mfx, mlev, err = call(mid, outs, scratch, [*args, mtens], (), (3, 4, 5), 4)
        edges = [across(to_a, GY, 0), across(to_b, GY, 1)]
        whole = shared(coarse, GY).reshape(32 * count, 128)
        args = [par, whole, mfx, mlev, err, *edges]
        outs = [(2, 12, 4, 128)]
        scratch = [(3, 18, MROWS, 128), (3, 18, MROWS, 128), (6, 3 * MROWS, 128)]
        inverse = (6, 32, 128)
        low = functools.partial(coarse_kernel, first)
        if first:
            error, cinv = call(low, [*outs, inverse], [*saved, inverse, *scratch], args, (2, 3, 4), (1,), 4)
        else:
            (error,) = call(low, outs, [*saved, *scratch], [*args, cinv], (2, 3, 4), (), 4)
        args = [par, flow, *layers, *edges, error, *beside(error, GY), lev, tens]
        scratch = [(9, *fine_shape), (9, *fine_shape), (3, *fine_shape), (3, *fine_shape)]
        scratch += [(3, 12, 16, 128), (3, 12, 16, 128), (3, 12, 16, 128)]
        (flow,) = call(post_kernel, [(3, 8, 8, 128)], scratch, args, (9, 10), (), 2)
    return flow


def solution(mesh):
    finer = Mesh(mesh.devices.reshape(4, 2, 8, 4), ("gx_0", "gx_1", "gy_0", "gy_1"))
    return jax.shard_map(
        body,
        mesh=finer,
        in_specs=(P(GX, GY, None), P(GX, GY, None), P(None, GX, GY, None)),
        out_specs=P(None, GX, GY, None),
        check_vma=False,
    )
```

```python
import functools

import jax
import jax.numpy as jnp
from jax import lax
from jax.experimental import pallas as pl
from jax.experimental.pallas import tpu as pltpu
from jax.sharding import Mesh
from jax.sharding import PartitionSpec as P


SWEEPS = 4
COARSE_SWEEPS = 12
CYCLES = 2
GX = ("gx_0", "gx_1")
GY = ("gy_0", "gy_1")

damping = 0.6
smooth_weight = 2.0
floor_grad = 0.5

NX, NY = 64, 256
ROWS = 24
NEAR = slice(4, 20)
WIDE = 20
MROWS = 16


def roll(v, shift, axis):
    return pltpu.roll(v, shift % v.shape[axis], axis)


def iota(shape, dim):
    return lax.broadcasted_iota(jnp.int32, shape, dim)


def face(a, b, scale):
    summed = a + b
    return (2.0 * scale) * a * b / jnp.where(summed > 0.0, summed, 1.0)


def inverse_sym(tensor, total):
    aaa = tensor[0] + total
    bbb = tensor[1]
    ccc = tensor[2]
    ddd = tensor[3] + total
    eee = tensor[4]
    fff = tensor[5] + total
    cof_a = ddd * fff - eee * eee
    cof_b = ccc * eee - bbb * fff
    cof_c = bbb * eee - ccc * ddd
    cof_d = aaa * fff - ccc * ccc
    cof_e = bbb * ccc - aaa * eee
    cof_f = aaa * ddd - bbb * bbb
    determinant = aaa * cof_a + bbb * cof_b + ccc * cof_c
    share = jnp.where(total > 0.0, damping / determinant, 0.0)
    return [cof * share for cof in (cof_a, cof_b, cof_c, cof_d, cof_e, cof_f)]


def apply_sym(m, v):
    return [
        m[0] * v[0] + m[1] * v[1] + m[2] * v[2],
        m[1] * v[0] + m[3] * v[1] + m[4] * v[2],
        m[2] * v[0] + m[4] * v[1] + m[5] * v[2],
    ]


def inflow(here, above, below, fx_up, fx_down, fy, fz):
    return (
        fx_up * above
        + fx_down * below
        + fy * roll(here, -1, 0)
        + roll(fy * here, 1, 0)
        + fz * roll(here, -1, 1)
        + roll(fz * here, 1, 1)
    )


def total_of(fx_up, fx_down, fy, fz):
    return fx_up + fx_down + fy + roll(fy, 1, 0) + fz + roll(fz, 1, 1)


def loop(low, high, turn):
    for index in range(low, high):
        turn(index)


def moved(pairs, sems):
    copies = [pltpu.make_async_copy(a, b, sems.at[k]) for k, (a, b) in enumerate(pairs)]
    for copy in copies:
        copy.start()
    return copies


def sides(par, which, shape):
    is_odd = (jnp.zeros(shape, jnp.int32) + (par[which] & 1)) == 1
    return (lambda a, b: jnp.where(is_odd, a, b)), (lambda a, b: jnp.where(is_odd, b, a))


def hat(distance):
    return jnp.maximum(1.0 - jnp.abs(distance), 0.0)


def thirds(a):
    high = a.astype(jnp.bfloat16)
    rest = a - high.astype(jnp.float32)
    middle = rest.astype(jnp.bfloat16)
    return [high, middle, (rest - middle.astype(jnp.float32)).astype(jnp.bfloat16)]


def dot(a, b):
    terms = jnp.concatenate(thirds(a), axis=0)
    got = jnp.dot(terms, b.astype(jnp.bfloat16), preferred_element_type=jnp.float32)
    n = a.shape[0]
    return got[0:n] + got[n : 2 * n] + got[2 * n :]


def dot_left(a, b):
    terms = jnp.concatenate(thirds(b), axis=1)
    got = jnp.dot(a.astype(jnp.bfloat16), terms, preferred_element_type=jnp.float32)
    n = b.shape[1]
    return got[:, 0:n] + got[:, n : 2 * n] + got[:, 2 * n :]


def fine_sweep(source, target, low, high, lev, tens):
    def turn(x):
        fx_up, fx_down = lev[0, x], lev[0, x - 1]
        fy, fz = lev[1, x], lev[2, x]
        here = [source[c, x] for c in range(3)]
        flux = [
            tens[6 + c, x]
            + inflow(here[c], source[c, x + 1], source[c, x - 1], fx_up, fx_down, fy, fz)
            for c in range(3)
        ]
        step = apply_sym([lev[3 + k, x] for k in range(6)], flux)
        for c in range(3):
            target[c, x] = (1.0 - damping) * here[c] + step[c]

    loop(low, high, turn)


def widen_kernel(par, own, xa, xb, wide, to_a, to_b):
    low_of, high_of = sides(par, 0, (8, 128))
    first_of, second_of = sides(par, 1, (4, 128))
    for f in range(own.shape[0]):
        for x in range(WIDE):
            if x < 6:
                v = low_of(xa[f, 2 + x], xb[f, 2 + x])
            elif x < 14:
                v = own[f, x - 6]
            else:
                v = high_of(xa[f, x - 14], xb[f, x - 14])
            wide[f, x] = v
            below, above = v[0:4], v[4:8]
            if 1 <= x < 19:
                to_a[f, x - 1] = first_of(below, above)
                to_b[f, x - 1] = second_of(below, above)
            if 5 <= x < 15:
                to_a[f, 13 + x] = first_of(above, below)
                to_b[f, 13 + x] = second_of(above, below)


def stack_rows(par, own, ya, yb, out, close):
    low_of, high_of = sides(par, 1, (4, 128))
    zero = jnp.zeros((4, 128), jnp.float32)
    for f in range(own.shape[0]):
        for x in range(WIDE):
            out[f, x, 8:16] = own[f, x]
            near = (ya[f, x - 1], yb[f, x - 1]) if 1 <= x < 19 else (zero, zero)
            far = (ya[f, 13 + x], yb[f, 13 + x]) if 5 <= x < 15 else (zero, zero)
            low, high = low_of(*near), high_of(*near)
            out[f, x, 0:4] = low_of(*far)
            out[f, x, 4:8] = low
            out[f, x, 16:20] = high
            out[f, x, 20:24] = high_of(*far)
            if f < 3:
                close[f, x, 0:4] = low
                close[f, x, 4:12] = own[f, x]
                close[f, x, 12:16] = high


def pre_kernel(first, *refs):
    if first:
        par, own, ya, yb, flow_out, msg, lev_far, tens_far, lev, tens, full, u0, u1, w, fy_low, even, odd, sums, sems = refs
    else:
        par, own, ya, yb, tens, flow_out, msg, lev_far, lev, full, u0, u1, w, fy_low, even, odd, sums, sems = refs
    shape = (ROWS, 128)
    lane = iota(shape, 1)
    last, start = lane == 127, lane == 0
    stack_rows(par, own, ya, yb, full, u0)
    near_last = iota((16, 128), 1) == 127

    def z_slope(v):
        return jnp.where(last, 0.0, roll(v, -1, 1)) - jnp.where(start, 0.0, roll(v, 1, 1))

    def y_slope(v):
        return roll(v, -1, 0) - roll(v, 1, 0)

    if first:

        def tensor_turn(x):
            mean = 0.5 * (full[3, x] + full[4, x])
            sx = 0.25 * ((full[3, x + 1] + full[4, x + 1]) - (full[3, x - 1] + full[4, x - 1]))
            sy = 0.5 * y_slope(mean)
            sz = 0.5 * z_slope(mean)
            change = full[4, x] - full[3, x]
            scale = 1.0 / (sx * sx + sy * sy + sz * sz + floor_grad)
            gx, gy, gz = scale * sx, scale * sy, scale * sz
            for k, v in enumerate((gx * sx, gx * sy, gx * sz, gy * sy, gy * sz, gz * sz)):
                tens[k, x] = v[NEAR]
            for k, v in enumerate((gx, gy, gz)):
                tens[6 + k, x] = (-v * change)[NEAR]

        loop(2, 18, tensor_turn)

    row = iota(shape, 0) + (par[1] * 8 - 8)
    inside_y = (row >= 0) & (row < NY)

    def weight_turn(x):
        total = jnp.ones(shape, jnp.float32)
        for c in range(3):
            v = full[c, x]
            for slope in (full[c, x + 1] - full[c, x - 1], y_slope(v), z_slope(v)):
                total = total + slope * slope
        place = x + (par[0] * 8 - 6)
        keep = jnp.where((place >= 0) & (place < NX), 1.0, 0.0)
        w[x] = jnp.where(inside_y, lax.rsqrt(total), 0.0) * keep

    loop(1, 19, weight_turn)

    def face_turn(x):
        v = w[x]
        near = v[NEAR]
        lev[0, x] = face(near, w[x + 1][NEAR], smooth_weight)
        if x > 1:
            along = face(v, roll(v, -1, 0), smooth_weight)
            lev[1, x] = along[NEAR]
            fy_low[x] = along[3:19]
            lev[2, x] = jnp.where(near_last, 0.0, face(near, roll(near, -1, 1), smooth_weight))

    loop(1, 18, face_turn)

    def inverse_turn(x):
        fz = lev[2, x]
        total = lev[0, x] + lev[0, x - 1] + lev[1, x] + fy_low[x] + fz + roll(fz, 1, 1)
        for k, v in enumerate(inverse_sym([tens[k, x] for k in range(6)], total)):
            lev[3 + k, x] = v

    loop(2, 18, inverse_turn)
    far = [(lev, lev_far), (tens, tens_far)] if first else [(lev, lev_far)]
    copies = moved(far, sems)
    bufs = (u0, u1)


    def first_turn(x):
        fx_up, fx_down = lev[0, x], lev[0, x - 1]
        fy, fz = lev[1, x], lev[2, x]
        here = [u0[c, x] for c in range(3)]
        flux = [
            tens[6 + c, x]
            + fx_up * u0[c, x + 1]
            + fx_down * u0[c, x - 1]
            + fy * full[c, x, 5:21]
            + fy_low[x] * full[c, x, 3:19]
            + fz * roll(here[c], -1, 1)
            + roll(fz * here[c], 1, 1)
            for c in range(3)
        ]
        step = apply_sym([lev[3 + k, x] for k in range(6)], flux)
        for c in range(3):
            u1[c, x] = (1.0 - damping) * here[c] + step[c]

    loop(2, 18, first_turn)
    for n in range(1, SWEEPS):
        fine_sweep(bufs[n % 2], bufs[(n + 1) % 2], 2 + n, 18 - n, lev, tens)

    def rest_at(x):
        fx_up, fx_down = lev[0, x], lev[0, x - 1]
        fy, fz = lev[1, x], lev[2, x]
        total = total_of(fx_up, fx_down, fy, fz)
        here = [u0[c, x] for c in range(3)]
        moved = apply_sym([tens[k, x] for k in range(6)], here)
        return [
            (
                tens[6 + c, x]
                + inflow(here[c], u0[c, x + 1], u0[c, x - 1], fx_up, fx_down, fy, fz)
                - moved[c]
                - total * here[c]
            )[4:12]
            for c in range(3)
        ]

    def rest_turn(m):
        x = 6 + 2 * m
        rest = [a + b for a, b in zip(rest_at(x), rest_at(x + 1))]
        pair = w[x] + w[x + 1]
        fields = rest + [pair[8:16], roll(pair, 2, 0)[8:16], pair[16:24]]
        if first:
            fields += [tens[k, x, 4:12] + tens[k, x + 1, 4:12] for k in range(6)]
        for k, v in enumerate(fields):
            stage = odd if k % 2 else even
            at = (k // 2) * 32 + m * 8
            stage[at : at + 8] = v

    loop(0, 4, rest_turn)
    for c in range(3):
        for k in range(8):
            flow_out[c, k] = u0[c, 6 + k, 4:12]
    square = (128, 128)
    into = iota(square, 0) // 2
    low = jnp.where(into == iota(square, 1), 0.125, 0.0)
    high = jnp.where(into + 64 == iota(square, 1), 0.125, 0.0)
    sums[...] = dot(even[...], low) + dot(odd[...], high)
    pairs = even.shape[0] // 32
    size = msg.shape[1]
    at = 0
    for p in range(pairs):
        if p == 2:
            v = sums[pl.ds(64, 4, stride=8), :] + sums[pl.ds(65, 4, stride=8), :]
            for s in range(8):
                msg[s, size - 8 : size - 4] = v
                msg[s, size - 4 : size] = v
            continue
        v = sums[pl.ds(p * 32, 16, stride=2), :] + sums[pl.ds(p * 32 + 1, 16, stride=2), :]
        for s in range(8):
            msg[s, at : at + 16] = v
        at += 16
    for copy in copies:
        copy.wait()


def wide_layers(par, own, xa, xb, place):
    low_of, high_of = sides(par, 0, (8, 128))
    for c in range(3):
        for k in range(4):
            place(c, k, low_of(xa[c, 4 + k], xb[c, 4 + k]))
            place(c, 12 + k, high_of(xa[c, k], xb[c, k]))
        for k in range(8):
            place(c, 4 + k, own[c, k])


def send_flow(par, flow, fa, fb, to_a, to_b):
    first_of, second_of = sides(par, 1, (4, 128))

    def place(c, k, v):
        to_a[c, k] = first_of(v[0:4], v[4:8])
        to_b[c, k] = second_of(v[0:4], v[4:8])

    wide_layers(par, flow, fa, fb, place)


def mid_sweep(source, target, mfx, mlev):
    def turn(x):
        fx_up, fx_down = mfx[x + 1], mfx[x]
        fy, fz = mlev[0, x], mlev[1, x]
        here = [source[c, x + 1] for c in range(3)]
        flux = [
            mlev[8 + c, x]
            + inflow(here[c], source[c, x + 2], source[c, x], fx_up, fx_down, fy, fz)
            for c in range(3)
        ]
        step = apply_sym([mlev[2 + k, x] for k in range(6)], flux)
        for c in range(3):
            target[c, x + 1] = (1.0 - damping) * here[c] + step[c]

    loop(0, 16, turn)
    seam(target)


def seam(field):
    for c in range(3):
        field[c, 0] = roll(field[c, 16], 64, 1)
        field[c, 17] = roll(field[c, 1], 64, 1)


def mid_kernel(first, *refs):
    if first:
        par, own, ya, yb, flow, fa, fb, msg, to_a, to_b, *refs = refs
        mfx_far, mlev_far, err_far, mtens_far, mfx, mlev, err, mtens, u1, w, stage, sems = refs
    else:
        par, own, ya, yb, flow, fa, fb, mtens, msg, to_a, to_b, *refs = refs
        mfx_far, mlev_far, err_far, mfx, mlev, err, u1, w, stage, sems = refs
    send_flow(par, flow, fa, fb, to_a, to_b)
    shape = (MROWS, 128)
    lane = iota(shape, 1)
    left = iota((8, 128), 1) < 64
    low_of, high_of = sides(par, 1, (8, 128))
    size = own.shape[1]
    zero4 = jnp.zeros((4, 128), jnp.float32)

    def split(a, b, which):
        if which:
            return jnp.where(left, roll(a, 64, 1), b)
        return jnp.where(left, a, roll(b, 64, 1))

    def fields_of(out, slot, pair, which):
        def turn(a):
            for kk in range(2):
                rows = slice(pair * 16 + kk * 8, pair * 16 + kk * 8 + 8)
                la, lb = low_of(ya[a, rows], yb[a, rows]), low_of(ya[a + 4, rows], yb[a + 4, rows])
                ha, hb = high_of(ya[a, rows], yb[a, rows]), high_of(ya[a + 4, rows], yb[a + 4, rows])
                for base, va, vb in ((1, la, lb), (5, own[a, rows], own[a + 4, rows]), (9, ha, hb)):
                    v = split(va, vb, which)
                    for k in range(2):
                        x = a * 4 + kk * 2 + k
                        if slot is None:
                            out[x, base : base + 4] = v[4 * k : 4 * k + 4]
                        else:
                            out[slot, x, base : base + 4] = v[4 * k : 4 * k + 4]

        loop(0, 4, turn)

    def clear_turn(x):
        for ref in (w,):
            ref[x, 0:1] = zero4[0:1]
            ref[x, 13:16] = zero4[0:3]
        for k in range(3):
            mlev[8 + k, x, 0:1] = zero4[0:1]
            mlev[8 + k, x, 13:16] = zero4[0:3]
        if first:
            for k in range(6):
                mtens[k, x, 0:1] = zero4[0:1]
                mtens[k, x, 13:16] = zero4[0:3]

    loop(0, 16, clear_turn)
    fields_of(mlev, 8, 0, 0)
    fields_of(mlev, 9, 0, 1)
    fields_of(mlev, 10, 1, 0)
    fields_of(w, None, 1, 1)
    if first:
        for k in range(6):
            fields_of(mtens, k, 2 + k // 2, k % 2)
    outer = slice(size - 8, size)
    for a in range(4):
        la, lb = low_of(ya[a, outer], yb[a, outer]), low_of(ya[a + 4, outer], yb[a + 4, outer])
        ha, hb = high_of(ya[a, outer], yb[a, outer]), high_of(ya[a + 4, outer], yb[a + 4, outer])
        lo, hi = split(la, lb, 0), split(ha, hb, 1)
        for k in range(4):
            w[a * 4 + k, 0:1] = lo[k : k + 1]
            w[a * 4 + k, 13:14] = hi[k : k + 1]

    scale = smooth_weight / 4.0
    stop = (lane == 63) | (lane == 127)

    def face_turn(x):
        v = w[x]
        mlev[0, x] = face(v, roll(v, -1, 0), scale)
        mlev[1, x] = jnp.where(stop, 0.0, face(v, roll(v, -1, 1), scale))

    loop(0, 16, face_turn)

    def across_turn(x):
        mfx[x + 1] = face(w[x], w[x + 1], scale)

    loop(0, 15, across_turn)
    seam_face = jnp.where(lane < 64, face(w[15], roll(w[0], 64, 1), scale), 0.0)
    mfx[16] = seam_face
    mfx[0] = roll(seam_face, 64, 1)

    def inverse_turn(x):
        total = total_of(mfx[x + 1], mfx[x], mlev[0, x], mlev[1, x])
        inv = inverse_sym([mtens[k, x] for k in range(6)], total)
        for k in range(6):
            mlev[2 + k, x] = inv[k]
        begin = apply_sym(inv, [mlev[8 + c, x] for c in range(3)])
        for c in range(3):
            u1[c, x + 1] = begin[c]

    loop(0, 16, inverse_turn)
    seam(u1)
    far = [(mfx, mfx_far), (mlev, mlev_far)]
    copies = moved(far + [(mtens, mtens_far)] if first else far, sems)
    bufs = (u1, err)
    for n in range(SWEEPS - 1):
        mid_sweep(bufs[n % 2], bufs[(n + 1) % 2], mfx, mlev)
    (err_copy,) = moved([(err, err_far)], sems.at[3:4])
    count = stage.shape[0] // 4
    stage[...] = jnp.zeros(stage.shape, jnp.float32)

    def rest_turn(a):
        sums = [jnp.zeros(shape, jnp.float32) for _ in range(9 if first else 3)]
        for k in range(4):
            x = a * 4 + k
            fx_up, fx_down = mfx[x + 1], mfx[x]
            fy, fz = mlev[0, x], mlev[1, x]
            total = total_of(fx_up, fx_down, fy, fz)
            here = [err[c, x + 1] for c in range(3)]
            moved = apply_sym([mtens[k, x] for k in range(6)], here)
            for c in range(3):
                sums[c] = sums[c] + (
                    mlev[8 + c, x]
                    + inflow(here[c], err[c, x + 2], err[c, x], fx_up, fx_down, fy, fz)
                    - moved[c]
                    - total * here[c]
                )
            if first:
                for q in range(6):
                    sums[3 + q] = sums[3 + q] + mtens[q, x]
        for q, v in enumerate(sums):
            stage[a * count + q : a * count + q + 1] = jnp.sum(v[5:9], axis=0, keepdims=True)

    loop(0, 4, rest_turn)
    for c in range(3):
        for x in range(16):
            v = err[c, x + 1, 5:9]
            to_a[3 + c, x] = v
            to_b[3 + c, x] = v
    square = (128, 128)
    z, to = iota(square, 0), iota(square, 1)
    gather = jnp.where((z // 64 == to // 64) & ((z % 64) // 4 == to % 64), 1.0 / 64.0, 0.0)
    mixed = dot(stage[...], gather)
    value = mixed[0:count]
    for a in range(1, 4):
        value = value + roll(mixed[a * count : (a + 1) * count], 16 * a, 1)
    value = value[0 : msg.shape[1]]
    for s in range(32):
        msg[s] = value
    for copy in [*copies, err_copy]:
        copy.wait()


def coarse_kernel(first, *refs):
    if first:
        par, whole, mfx_far, mlev_far, err_far, ea, eb, out, cinv_far, mfx, mlev, err, cinv, u0, u1, lifted, sems = refs
    else:
        par, whole, mfx_far, mlev_far, err_far, ea, eb, cinv, out, mfx, mlev, err, u0, u1, lifted, sems = refs
    copies = moved([(mfx_far, mfx), (mlev_far, mlev), (err_far, err)], sems)
    count = whole.shape[0] // 32
    grid = (32, 128)
    row, lane = iota(grid, 0), iota(grid, 1)
    cx, cz = lane // 16, lane % 16
    scale = smooth_weight / 64.0
    one = lambda cond: jnp.where(cond, scale, 0.0)
    ups = (one(cx < 7), one(cx > 0), one(row < 31), one(row > 0), one(cz < 15), one(cz > 0))
    total = ups[0] + ups[1] + ups[2] + ups[3] + ups[4] + ups[5]
    if first:
        inv = inverse_sym([whole[pl.ds(3 + k, 32, stride=count), :] for k in range(6)], total)
        for k in range(6):
            cinv[k] = inv[k]
        copies += moved([(cinv, cinv_far)], sems.at[3:4])
    inv = [cinv[k] for k in range(6)]
    source = [whole[pl.ds(c, 32, stride=count), :] for c in range(3)]

    def turn(index, now):
        flux = []
        for c in range(3):
            v = now[c]
            flux.append(
                source[c]
                + ups[0] * roll(v, -16, 1)
                + ups[1] * roll(v, 16, 1)
                + ups[2] * roll(v, -1, 0)
                + ups[3] * roll(v, 1, 0)
                + ups[4] * roll(v, -1, 1)
                + ups[5] * roll(v, 1, 1)
            )
        step = apply_sym(inv, flux)
        return tuple((1.0 - damping) * now[c] + step[c] for c in range(3))

    correction = lax.fori_loop(0, COARSE_SWEEPS - 1, turn, tuple(apply_sym(inv, source)))

    shape = (MROWS, 32)
    place = (iota(shape, 0) + (par[1] * 4 - 5)).astype(jnp.float32) * 0.25 - 0.375
    along = hat(place - iota(shape, 1).astype(jnp.float32))
    rows = jnp.concatenate([dot_left(along, correction[c]) for c in range(3)], axis=0)
    square = (128, 128)
    src, to = iota(square, 0), iota(square, 1)
    depth = hat((to % 64).astype(jnp.float32) * 0.25 - 0.375 - (src % 16).astype(jnp.float32))
    for a in range(4):
        spread = jnp.where(src // 16 == a + 4 * (to // 64), depth, 0.0)
        lifted[a + 1] = dot(rows, spread)
    halves = iota((3 * MROWS, 128), 1) < 64
    lifted[0] = jnp.where(halves, 0.0, roll(lifted[4], 64, 1))
    lifted[5] = jnp.where(halves, roll(lifted[1], 64, 1), 0.0)

    for copy in copies:
        copy.wait()
    low_of, high_of = sides(par, 1, (4, 128))
    zero = jnp.zeros((MROWS, 128), jnp.float32)
    for x in range(16):
        a, d = x // 4, x % 4
        t = (d + 0.5) / 4 - 0.5
        other = a if t < 0 else a + 2
        added = (1.0 - abs(t)) * lifted[a + 1] + abs(t) * lifted[other]
        for c in range(3):
            u0[c, x + 1] = zero
            u0[c, x + 1, 1:5] = low_of(ea[3 + c, x], eb[3 + c, x])
            u0[c, x + 1, 5:9] = err[c, x + 1, 5:9]
            u0[c, x + 1, 9:13] = high_of(ea[3 + c, x], eb[3 + c, x])
            u0[c, x + 1] = u0[c, x + 1] + added[c * MROWS : (c + 1) * MROWS]
    seam(u0)
    bufs = (u0, u1)
    for n in range(SWEEPS):
        mid_sweep(bufs[n % 2], bufs[(n + 1) % 2], mfx, mlev)

    left = iota((4, 128), 1) < 64
    for b in range(3):
        block = par[0] + (b - 1)
        there = jnp.where((block >= 0) & (block < 8), 1.0, 0.0)
        block = jnp.clip(block, 0, 7)
        upper = (jnp.zeros((4, 128), jnp.int32) + block // 4) == 1
        for k in range(4):
            x = (block % 4) * 4 + k + 1
            v = [u0[c, x, 5:9] for c in range(3)]
            v = [(a, roll(a, 64, 1)) for a in v]
            to_left = [jnp.where(upper, turned, a) for a, turned in v]
            to_right = [jnp.where(upper, a, turned) for a, turned in v]
            out[0, b * 4 + k] = jnp.where(left, to_left[0], to_right[1]) * there
            out[1, b * 4 + k] = jnp.where(left, to_left[2], 0.0) * there


def post_kernel(par, flow, fa, fb, ya, yb, mine, ea, eb, lev_far, tens_far, out, lev, tens, u0, u1, mixed, lifted, tall, sems):
    copies = moved(
        [(lev_far.at[:, 2:17], lev.at[:, 2:17]), (tens_far.at[6:9, 3:17], tens.at[6:9, 3:17])], sems
    )
    low_of, high_of = sides(par, 1, (4, 128))
    zero = jnp.zeros((4, 128), jnp.float32)

    def place(c, k, v):
        u0[c, 2 + k, 4:12] = v

    wide_layers(par, flow, fa, fb, place)

    def edge_turn(k):
        for c in range(3):
            u0[c, 2 + k, 0:4] = low_of(ya[c, k], yb[c, k])
            u0[c, 2 + k, 12:16] = high_of(ya[c, k], yb[c, k])

    loop(0, 16, edge_turn)
    for x in range(12):
        for p in range(2):
            v = [low_of(ea[p, x], eb[p, x]), mine[p, x], high_of(ea[p, x], eb[p, x])]
            for q in range(3):
                mixed[2 * p, x, 4 * q : 4 * q + 4] = v[q]
            mixed[2 * p, x, 12:16] = zero
    square = (128, 128)
    src, to = iota(square, 0), iota(square, 1)
    place = to.astype(jnp.float32) * 0.5 - 0.25
    depth = hat(place - (src % 64).astype(jnp.float32))
    low = jnp.where(src < 64, depth, 0.0)
    high = jnp.where(src < 64, 0.0, depth)
    for c in range(3):
        v = mixed[2 * (c // 2)].reshape(12 * 16, 128)
        lifted[c] = dot(v, high if c == 1 else low).reshape(12, 16, 128)

    def tall_turn(x):
        for c in range(3):
            v = lifted[c, x]
            tall[c, x, pl.ds(0, 8, stride=2), :] = (0.75 * v + 0.25 * roll(v, 1, 0))[2:10]
            tall[c, x, pl.ds(1, 8, stride=2), :] = (0.75 * v + 0.25 * roll(v, -1, 0))[2:10]

    loop(1, 11, tall_turn)

    def add_turn(m):
        for c in range(3):
            a, b, d = tall[c, m - 1], tall[c, m], tall[c, m + 1]
            x = 2 * m - 2
            u0[c, x] = u0[c, x] + (0.75 * b + 0.25 * a)
            u0[c, x + 1] = u0[c, x + 1] + (0.75 * b + 0.25 * d)

    loop(2, 10, add_turn)
    for copy in copies:
        copy.wait()
    bufs = (u0, u1)
    for n in range(SWEEPS):
        fine_sweep(bufs[n % 2], bufs[(n + 1) % 2], 3 + n, 17 - n, lev, tens)
    for c in range(3):
        for k in range(8):
            out[c, k] = u0[c, 6 + k, 4:12]


def f32(*shape):
    return jax.ShapeDtypeStruct(shape, jnp.float32)


def call(kernel, outs, scratch, args, far_in=(), far_out=(), sems=0):
    near, far = pl.BlockSpec(memory_space=pltpu.VMEM), pl.BlockSpec(memory_space=pltpu.HBM)
    args = [pltpu.with_memory_space_constraint(v, pltpu.HBM) if k in far_in else v for k, v in enumerate(args)]
    specs = [pl.BlockSpec(memory_space=pltpu.SMEM)]
    specs += [far if k in far_in else near for k in range(1, len(args))]
    scratch_shapes = [pltpu.VMEM(shape, jnp.float32) for shape in scratch]
    if sems:
        scratch_shapes.append(pltpu.SemaphoreType.DMA((sems,)))
    return pl.pallas_call(
        kernel,
        in_specs=specs,
        out_specs=[far if k in far_out else near for k in range(len(outs))],
        out_shape=[pltpu.HBM(shape, jnp.float32) if k in far_out else f32(*shape) for k, shape in enumerate(outs)],
        scratch_shapes=scratch_shapes,
        compiler_params=pltpu.CompilerParams(vmem_limit_bytes=24 * 2**20),
        cost_estimate=pl.CostEstimate(flops=20_000_000, bytes_accessed=1_000_000, transcendentals=0),
    )(*args)


def pairs_of(size, start):
    pairs = []
    for k in range(start, size - 1, 2):
        pairs += [(k, k + 1), (k + 1, k)]
    return pairs


def across(field, axes, start):
    return lax.ppermute(field, axes, pairs_of(lax.axis_size(axes), start))


def beside(field, axes):
    return [across(field, axes, 0), across(field, axes, 1)]


def shared(message, axes):
    return lax.all_to_all(message, axes, 0, 0, tiled=True)


def body(first_image, second_image, start_flow):
    par = jnp.stack([lax.axis_index(GX), lax.axis_index(GY)]).astype(jnp.int32)
    block = jnp.concatenate([start_flow, first_image[None], second_image[None]])
    flow = start_flow
    tens = mtens = cinv = None
    tall_shape, fine_shape, mid_shape = (WIDE, ROWS, 128), (WIDE, 16, 128), (16, MROWS, 128)
    for cycle in range(CYCLES):
        first = cycle == 0
        sent = block if first else flow
        fields = sent.shape[0]
        args = [par, sent, *beside(sent, GX)]
        outs = [(fields, WIDE, 8, 128), (fields, 28, 4, 128), (fields, 28, 4, 128)]
        wide, to_a, to_b = call(widen_kernel, outs, [], args)
        size = 88 if first else 40
        stage = (6 if first else 3) * 32
        outs = [(3, 8, 8, 128), (8, size, 128), (9, *fine_shape)]
        scratch = [(9, *fine_shape)] * (2 if first else 1)
        scratch += [(fields, *tall_shape), (3, *fine_shape), (3, *fine_shape), tall_shape, fine_shape]
        scratch += [(stage, 128)] * 3
        args = [par, wide, across(to_a, GY, 0), across(to_b, GY, 1)]
        pre = functools.partial(pre_kernel, first)
        if first:
            flow, message, lev, tens = call(pre, [*outs, (9, *fine_shape)], scratch, args, (), (2, 3), 2)
        else:
            flow, message, lev = call(pre, outs, scratch, [*args, tens], (), (2,), 2)
        layers = beside(flow, GX)
        mids = shared(message, GX)
        args = [par, mids, *beside(mids, GY), flow, *layers]
        count, padded = (12, 16) if first else (4, 8)
        sides_shape = (6, 16, 4, 128)
        saved = [(17, MROWS, 128), (11, *mid_shape), (3, 18, MROWS, 128)]
        outs = [(32, count, 128), sides_shape, sides_shape, *saved]
        scratch = [*saved, *([(6, *mid_shape)] if first else []), (3, 18, MROWS, 128), mid_shape, (4 * padded, 128)]
        mid = functools.partial(mid_kernel, first)
        if first:
            coarse, to_a, to_b, mfx, mlev, err, mtens = call(
                mid, [*outs, (6, *mid_shape)], scratch, args, (), (3, 4, 5, 6), 4
            )
        else:
            coarse, to_a, to_b, mfx, mlev, err = call(mid, outs, scratch, [*args, mtens], (), (3, 4, 5), 4)
        edges = [across(to_a, GY, 0), across(to_b, GY, 1)]
        whole = shared(coarse, GY).reshape(32 * count, 128)
        args = [par, whole, mfx, mlev, err, *edges]
        outs = [(2, 12, 4, 128)]
        scratch = [(3, 18, MROWS, 128), (3, 18, MROWS, 128), (6, 3 * MROWS, 128)]
        inverse = (6, 32, 128)
        low = functools.partial(coarse_kernel, first)
        if first:
            error, cinv = call(low, [*outs, inverse], [*saved, inverse, *scratch], args, (2, 3, 4), (1,), 4)
        else:
            (error,) = call(low, outs, [*saved, *scratch], [*args, cinv], (2, 3, 4), (), 4)
        args = [par, flow, *layers, *edges, error, *beside(error, GY), lev, tens]
        scratch = [(9, *fine_shape), (9, *fine_shape), (3, *fine_shape), (3, *fine_shape)]
        scratch += [(3, 12, 16, 128), (3, 12, 16, 128), (3, 12, 16, 128)]
        (flow,) = call(post_kernel, [(3, 8, 8, 128)], scratch, args, (9, 10), (), 2)
    return flow


def solution(mesh):
    finer = Mesh(mesh.devices.reshape(4, 2, 8, 4), ("gx_0", "gx_1", "gy_0", "gy_1"))
    return jax.shard_map(
        body,
        mesh=finer,
        in_specs=(P(GX, GY, None), P(GX, GY, None), P(None, GX, GY, None)),
        out_specs=P(None, GX, GY, None),
        check_vma=False,
    )
```
